256 devices in a mesh: img: 2 (over z), ga: 16 (over y, core), band: 8 (over x).
Axes of the slice: x: 8, y: 8, z: 2, core: 2. Of those that a mesh axis runs over, the one named last changes fastest.
The devices are a block of a 8x8x16 slice.
Arguments:
- orbitals: bfloat16 [1536, 49152], P(('img', 'band'), 'ga'), parts along dimension 0, as said below
- kernel: float32 [49152], P('ga'), may hold values from 0.3 to 3
- block_vectors: bfloat16 [512, 49152], P(('img', 'band'), 'ga'), parts along dimension 0
Outputs:
- ace_vectors: bfloat16 [1536, 49152], P(('img', 'band'), 'ga'), parts along dimension 0
- exchange_block: bfloat16 [512, 49152], P(('img', 'band'), 'ga'), parts along dimension 0
The draws below stay inside these ranges and needn't reach their ends.
There are 2 independent parts, one for each index of `img`. The reference program is written for one: setup_inputs(seed, part) draws one part's arguments, and reference() takes and returns one part's arrays. A program takes and returns all parts, laid end to end along the dimension named above; an argument that names none is the same for every part. Nothing has to cross between parts.
Inputs may be any that keep to these rules, and one draw needn't show every extreme that they name: `orbitals`: the bands of one image are linearly independent, and the block lies largely in their span.
All inputs are finite; a program needn't handle non-finite values.
Results may differ from the reference program's by a relative error of at most 0.02.
Values may be sent and summed in bfloat16 or wider, within the bound.
No kernel may reach another device: no remote copies, remote signals or barrier semaphores. Data moves between devices by JAX's collectives and lax.ppermute only.
A program may use at most 64 MiB of HBM per device.

```python
import math
import jax
import jax.numpy as jnp
from jax import lax

NB = 768
NBLK = 256
NG = 49152


def orbital_pair(key):
    independent = jax.random.normal(jax.random.fold_in(key, 11), (NB, NG), jnp.float32)
    mixing = jax.random.normal(jax.random.fold_in(key, 12), (NB, NB), jnp.float32) * (0.4 / math.sqrt(NB))
    orbital_rows = independent + jnp.dot(mixing, independent, precision=lax.Precision.HIGHEST)
    mixture = jax.random.normal(jax.random.fold_in(key, 13), (NBLK, NB), jnp.float32) / math.sqrt(NB)
    residue = jax.random.normal(jax.random.fold_in(key, 14), (NBLK, NG), jnp.float32)
    block_rows = jnp.dot(mixture, orbital_rows, precision=lax.Precision.HIGHEST) + 0.5 * residue
    return (orbital_rows, block_rows)


def draw_orbitals(key, part):
    return orbital_pair(key)[0].astype(jnp.bfloat16)


def draw_block_vectors(key, part):
    return orbital_pair(key)[1].astype(jnp.bfloat16)


def steps_of(rng, extent, pieces, least, high):
    gain, own = 1.0, jax.random.fold_in(rng, 6)
    for position, blocks in pieces:
        heights = jnp.exp(jax.random.uniform(jax.random.fold_in(own, position), (blocks,), jnp.float32, least / len(pieces), high / len(pieces)))
        gain = gain * jnp.repeat(heights, extent[position] // blocks).reshape([-1 if axis == position else 1 for axis in range(len(extent))])
    return gain


def setup_inputs(seed: int = 0, part: int = 0) -> dict:
    arg_keys = jax.random.split(jax.random.key(seed), 4)
    part_keys = jax.random.split(jax.random.fold_in(arg_keys[3], part), 4)
    orbitals = draw_orbitals(jax.random.fold_in(jax.random.fold_in(arg_keys[3], part), 71), part)
    kernel = jnp.clip(jnp.exp(math.log(3.0) - 2.3025851 * jax.random.uniform(arg_keys[1], (NG,), jnp.float32) ** steps_of(arg_keys[1], (NG,), ((0, 16),), -0.2, 0.2)), 0.3, 3.0)
    block_vectors = draw_block_vectors(jax.random.fold_in(jax.random.fold_in(arg_keys[3], part), 71), part)
    return {"orbitals": orbitals, "kernel": kernel, "block_vectors": block_vectors}


def reference(orbitals, kernel, block_vectors):
    weighted = (-(orbitals.astype(jnp.float32) * kernel[None, :])).astype(jnp.bfloat16)
    margin = -lax.dot_general(orbitals.astype(jnp.float32), weighted.astype(jnp.float32), (((1,), (1,)), ((), ())), preferred_element_type=jnp.float32) / NG
    factor = jnp.linalg.cholesky(margin)
    projector = lax.linalg.triangular_solve(factor, weighted.astype(jnp.float32), left_side=True, lower=True)
    coupling = jnp.dot(projector, block_vectors.astype(jnp.float32).T, precision=lax.Precision.HIGHEST) / NG
    applied = -lax.dot_general(coupling, projector, (((0,), (0,)), ((), ())), precision=lax.Precision.HIGHEST)
    return (projector.astype(jnp.bfloat16), applied.astype(jnp.bfloat16))
```

```python
import functools

import jax
import jax.numpy as jnp
from jax import lax
from jax.experimental import pallas as pl
from jax.experimental.pallas import tpu as pltpu
from jax.sharding import Mesh
from jax.sharding import PartitionSpec as P

SUB = 8
BLK = 128
TILE = 512


def split(a):
    hi = a.astype(jnp.bfloat16)
    return hi, (a - hi.astype(jnp.float32)).astype(jnp.bfloat16)


def dot3(a, b, dims):
    (ah, al), (bh, bl) = a, b
    dot = functools.partial(
        lax.dot_general, dimension_numbers=(dims, ((), ())), preferred_element_type=jnp.float32
    )
    return dot(ah, bh) + (dot(ah, bl) + dot(al, bh))


def wide(x):
    return jnp.broadcast_to(x, (SUB, BLK))


def inverse_of_factor(rows, inv):
    sub = lax.broadcasted_iota(jnp.int32, (SUB, BLK), 0)
    for p in range(len(rows)):
        k = p * SUB
        v, g = rows[p], inv[p]
        cols = [wide(v[:, k + j : k + j + 1]) for j in range(SUB)]
        scale, mult, us, gs = [], {}, [], []
        for j in range(SUB):
            r = lax.rsqrt(wide(cols[j][j : j + 1]))
            lj = cols[j] * r
            for m in range(j + 1, SUB):
                mult[j, m] = wide(lj[m : m + 1])
                cols[m] = cols[m] - lj * mult[j, m]
            u, w = wide(v[j : j + 1]) * r, wide(g[j : j + 1]) * r
            below = jnp.where(sub > j, lj, 0.0)
            v = jnp.where(sub == j, u, v - below * u)
            g = jnp.where(sub == j, w, g - below * w)
            scale.append(r)
            us.append(u)
            gs.append(w)
        rows[p], inv[p] = v, g
        for q in range(p + 1, len(rows)):
            c = [wide(rows[q][:, k + j : k + j + 1]) for j in range(SUB)]
            a, b = rows[q], inv[q]
            for j in range(SUB):
                lj = c[j] * scale[j]
                for m in range(j + 1, SUB):
                    c[m] = c[m] - lj * mult[j, m]
                a = a - lj * us[j]
                b = b - lj * gs[j]
            rows[q], inv[q] = a, b
    return inv


def eliminate(a, g_ref, r_ref):
    blocks = a.shape[0] // BLK
    row = lax.broadcasted_iota(jnp.int32, (SUB, BLK), 0)
    col = lax.broadcasted_iota(jnp.int32, (SUB, BLK), 1)

    def step(b, _):
        at = pl.multiple_of(b * BLK, BLK)
        here = pl.ds(at, BLK)
        rows = [
            a[pl.ds(pl.multiple_of(at + SUB * i, SUB), SUB), here] for i in range(BLK // SUB)
        ]
        inv = [jnp.where(col == row + SUB * i, 1.0, 0.0) for i in range(BLK // SUB)]
        for i, g in enumerate(inverse_of_factor(rows, inv)):
            g_ref[SUB * i : SUB * (i + 1), :] = g
        g = g_ref[...]
        r = dot3(split(g), split(a[here, :]), ((1,), (0,)))
        r_ref[...] = r
        a[here, :] = r
        a[here, here] = g
        rb = split(a[here, :])

        def below(i, _):
            them = pl.ds(pl.multiple_of(i * BLK, BLK), BLK)
            update = dot3(split(r_ref[:, them]), rb, ((0,), (0,)))
            a[them, here] = jnp.zeros((BLK, BLK), jnp.float32)
            a[them, :] = a[them, :] - update
            return 0

        lax.fori_loop(b + 1, blocks, below, 0)
        return 0

    lax.fori_loop(0, blocks, step, 0)


def coefficients_kernel(at_ref, m_ref, s_ref, o_ref, a_ref, g_ref, r_ref):
    n = a_ref.shape[0]
    own = o_ref.shape[0] // 2 - s_ref.shape[0]
    a_ref[...] = m_ref[...].astype(jnp.float32)
    eliminate(a_ref, g_ref, r_ref)
    row = lax.broadcasted_iota(jnp.int32, (n, n), 0)
    col = lax.broadcasted_iota(jnp.int32, (n, n), 1)
    a_ref[...] = jnp.where(row >= col, a_ref[...], 0.0)
    inverse = split(a_ref[...])
    coupling = dot3(split(s_ref[...]), inverse, ((1,), (1,)))
    applied = -dot3(split(coupling), inverse, ((1,), (0,)))
    first = pl.multiple_of(at_ref[0] * own, SUB)
    half = o_ref.shape[0] // 2
    hi, lo = split(a_ref[pl.ds(first, own), :])
    o_ref[:own, :] = hi
    o_ref[half : half + own, :] = lo
    hi, lo = split(applied)
    o_ref[own:half, :] = hi
    o_ref[half + own :, :] = lo


def coefficients(at, margin, overlap, own):
    n = margin.shape[0]
    rows = own + overlap.shape[0]
    vmem = pl.BlockSpec(memory_space=pltpu.VMEM)
    return pl.pallas_call(
        coefficients_kernel,
        out_shape=jax.ShapeDtypeStruct((2 * rows, n), jnp.bfloat16),
        in_specs=[pl.BlockSpec(memory_space=pltpu.SMEM), vmem, vmem],
        out_specs=vmem,
        scratch_shapes=[
            pltpu.VMEM((n, n), jnp.float32),
            pltpu.VMEM((BLK, BLK), jnp.float32),
            pltpu.VMEM((BLK, n), jnp.float32),
        ],
        name="coefficients",
    )(at, margin, overlap)


def outputs_kernel(own, c_ref, *refs):
    pieces, (p_ref, x_ref), w_ref = refs[:-3], refs[-3:-1], refs[-1]
    at = 0
    for piece in pieces:
        w_ref[at : at + piece.shape[0], :] = piece[...]
        at += piece.shape[0]
    both = jnp.dot(c_ref[...], w_ref[...], preferred_element_type=jnp.float32)
    half = both.shape[0] // 2
    out = (both[:half] + both[half:]).astype(jnp.bfloat16)
    p_ref[...] = out[:own]
    x_ref[...] = out[own:]


def outputs(coefs, pieces, own):
    half, n = coefs.shape[0] // 2, coefs.shape[1]
    cols = pieces[0].shape[1]
    tile = lambda rows: pl.BlockSpec((rows, TILE), lambda i: (0, i))
    return pl.pallas_call(
        functools.partial(outputs_kernel, own),
        grid=(cols // TILE,),
        in_specs=[pl.BlockSpec(coefs.shape, lambda i: (0, 0))] + [tile(p.shape[0]) for p in pieces],
        out_specs=[tile(own), tile(half - own)],
        out_shape=[
            jax.ShapeDtypeStruct((own, cols), jnp.bfloat16),
            jax.ShapeDtypeStruct((half - own, cols), jnp.bfloat16),
        ],
        scratch_shapes=[pltpu.VMEM((n, TILE), jnp.bfloat16)],
        name="outputs",
    )(coefs, *pieces)


def ring_gather(shard):
    count = lax.axis_size("band")
    right = [(i, (i + 1) % count) for i in range(count)]
    left = [(i, (i - 1) % count) for i in range(count)]
    mid = shard.shape[0] // 2
    halves = [shard[:mid], shard[mid:]]
    got = [[None, None] for _ in range(count)]
    got[0] = list(halves)
    far = count // 2
    moving = {("r", 0): halves[0], ("l", 1): halves[1], ("r", 1): halves[1], ("l", 0): halves[0]}
    for s in range(1, far + 1):
        for (way, h), piece in list(moving.items()):
            if s == far and (way, h) in (("r", 1), ("l", 0)):
                continue
            piece = lax.ppermute(piece, "band", right if way == "r" else left)
            moving[way, h] = piece
            got[(count - s if way == "r" else s) % count][h] = piece
    return got


def to_all(shard, axis):
    count = lax.axis_size(axis)
    return lax.all_to_all(
        jnp.broadcast_to(shard[None], (count, *shard.shape)), axis, 0, 0, tiled=True
    )


def shards(orbitals, kernel, block_vectors):
    band = lax.axis_index("band")
    core = lax.axis_index("core")
    count = lax.axis_size("band")
    total = orbitals.shape[1] * lax.axis_size("y") * lax.axis_size("core")
    own, mine = orbitals.shape[0], block_vectors.shape[0]
    ho, hb = own // 2, mine // 2
    swap = [(0, 1), (1, 0)]

    weighted = (-(orbitals.astype(jnp.float32) * kernel[None, :])).astype(jnp.bfloat16)
    got = ring_gather(weighted)

    left = jnp.concatenate(
        [orbitals[:ho], block_vectors[:hb], orbitals[ho:], block_vectors[hb:]], axis=0
    )
    parts = [
        lax.dot_general(left, half, (((1,), (1,)), ((), ())), preferred_element_type=jnp.float32)
        for pair in got
        for half in pair
    ]
    partial = jnp.concatenate(parts + parts, axis=1)
    n = own * count
    partial = lax.dynamic_slice_in_dim(partial, (count - band) * own, n, 1)

    rows = ho + hb
    kept = lax.dynamic_slice_in_dim(partial, core * rows, rows, 0)
    sent = lax.dynamic_slice_in_dim(partial, (1 - core) * rows, rows, 0)
    kept = kept + lax.ppermute(sent, "core", swap)
    summed = to_all(kept.astype(jnp.bfloat16), "y").astype(jnp.float32).sum(axis=0) / total
    margin_rows = to_all((-summed[:ho]).astype(jnp.bfloat16), "band")
    other_rows = lax.ppermute(margin_rows, "core", swap)
    overlap = summed[ho:]
    other = lax.ppermute(overlap, "core", swap)
    first = core == 0
    margin = jnp.concatenate(
        [
            jnp.where(first, margin_rows, other_rows)[:, None],
            jnp.where(first, other_rows, margin_rows)[:, None],
        ],
        axis=1,
    ).reshape(n, n)
    overlap = jnp.concatenate(
        [jnp.where(first, overlap, other), jnp.where(first, other, overlap)], axis=0
    )
    coefs = coefficients(band[None], margin, overlap, own)
    coefs = lax.dynamic_slice_in_dim(
        jnp.concatenate([coefs, coefs], axis=1), band * own, n, 1
    )
    return tuple(outputs(coefs, [half for pair in got for half in pair], own))


def solution(mesh):
    images, ga, bands = (mesh.shape[a] for a in ("img", "ga", "band"))
    split_mesh = Mesh(
        mesh.devices.reshape(images, ga // 2, 2, bands), ("img", "y", "core", "band")
    )
    rows, cols = ("img", "band"), ("y", "core")
    return jax.shard_map(
        shards,
        mesh=split_mesh,
        in_specs=(P(rows, cols), P(cols), P(rows, cols)),
        out_specs=(P(rows, cols), P(rows, cols)),
        check_vma=False,
    )
```

```python
import functools

import jax
import jax.numpy as jnp
from jax import lax
from jax.experimental import pallas as pl
from jax.experimental.pallas import tpu as pltpu
from jax.sharding import Mesh
from jax.sharding import PartitionSpec as P

SUB = 8
BLK = 128
TILE = 512


def split(a):
    hi = a.astype(jnp.bfloat16)
    return hi, (a - hi.astype(jnp.float32)).astype(jnp.bfloat16)


def dot3(a, b, dims):
    (ah, al), (bh, bl) = a, b
    dot = functools.partial(
        lax.dot_general, dimension_numbers=(dims, ((), ())), preferred_element_type=jnp.float32
    )
    return dot(ah, bh) + (dot(ah, bl) + dot(al, bh))


def wide(x):
    return jnp.broadcast_to(x, (SUB, BLK))


def lanes(x, k):
    return [wide(x[:, k + j : k + j + 1]) for j in range(SUB)]


def total_of(terms):
    while len(terms) > 1:
        odd = [terms[-1]] if len(terms) % 2 else []
        terms = [a + b for a, b in zip(terms[::2], terms[1::2])] + odd
    return terms[0]


def inverse_of_factor(rows, inv):
    sub = lax.broadcasted_iota(jnp.int32, (SUB, BLK), 0)
    at = [sub == j for j in range(SUB)]
    cols = lanes(rows[0], 0)
    for p in range(len(rows)):
        k = p * SUB
        v, g = rows[p], inv[p]
        last = p + 1 == len(rows)
        if not last:
            ahead, below = lanes(rows[p + 1], k + SUB), lanes(rows[p + 1], k)
        out, unit, recips = g, {}, []
        for j in range(SUB):
            pivot, cj = wide(cols[j][j : j + 1]), cols[j]
            recip = 1.0 / pivot
            recips.append(recip)
            for m in range(j + 1, SUB):
                t = wide(cols[m][j : j + 1]) * recip
                unit[j, m] = t
                cols[m] = jnp.where(at[j], t, cols[m] - cj * t)
            gj = wide(g[j : j + 1])
            out = jnp.where(at[j], gj * lax.rsqrt(pivot), out)
            vj, gj = wide(v[j : j + 1]) * recip, gj * recip
            v = jnp.where(at[j], vj, v - cj * vj)
            g = jnp.where(at[j], gj, g - cj * gj)
        inv[p] = out
        if last:
            break
        lower = list(below)
        for j in range(SUB):
            for m in range(j + 1, SUB):
                lower[m] = lower[m] - lower[j] * unit[j, m]
        scaled = [lower[j] * recips[j] for j in range(SUB)]
        cols = [
            ahead[m] - total_of([lower[j] * wide(scaled[j][m : m + 1]) for j in range(SUB)])
            for m in range(SUB)
        ]
        vs = [wide(v[j : j + 1]) for j in range(SUB)]
        gs = [wide(g[j : j + 1]) for j in range(SUB)]
        for q in range(p + 1, len(rows)):
            c = below if q == p + 1 else lanes(rows[q], k)
            rows[q] = rows[q] - total_of([c[j] * vs[j] for j in range(SUB)])
            inv[q] = inv[q] - total_of([c[j] * gs[j] for j in range(SUB)])
    return inv


def eliminate(a, d_ref, g_ref, r_ref):
    blocks = a.shape[0] // BLK
    row = lax.broadcasted_iota(jnp.int32, (SUB, BLK), 0)
    col = lax.broadcasted_iota(jnp.int32, (SUB, BLK), 1)
    groups = range(BLK // SUB)
    rows_of = ((0,), (0,))

    def block(i):
        return pl.ds(pl.multiple_of(i * BLK, BLK), BLK)

    d_ref[...] = a[:BLK, :BLK]
    r_ref[...] = jnp.zeros(r_ref.shape, jnp.float32)

    def step(b, _):
        rows = [d_ref[SUB * i : SUB * (i + 1), :] for i in groups]
        inv = [jnp.where(col == row + SUB * i, 1.0, 0.0) for i in groups]
        for i, g in enumerate(inverse_of_factor(rows, inv)):
            g_ref[SUB * i : SUB * (i + 1), :] = g
        r = split(r_ref[...])
        before = block(lax.rem(b + blocks - 1, blocks))
        for i in range(blocks - 1):
            them = block(lax.rem(b + i, blocks))
            live = jnp.logical_and(b > 0, b + i < blocks)
            factor = jnp.where(live, r_ref[:, them], 0.0)
            a[them, before] = jnp.where(live, 0.0, a[them, before])
            a[them, :] = a[them, :] - dot3(split(factor), r, rows_of)
        here, after = block(b), block(jnp.minimum(b + 1, blocks - 1))
        g = g_ref[...]
        r_ref[...] = dot3(split(g), split(a[here, :]), ((1,), (0,)))
        factor = split(r_ref[:, after])
        d_ref[...] = a[after, after] - dot3(factor, factor, rows_of)
        r_ref[:, here] = g
        a[here, :] = r_ref[...]
        return 0

    lax.fori_loop(0, blocks, step, 0)


def project_kernel(count, *refs):
    pieces = refs[4 : 4 + 2 * count]
    where_ref, mine_ref, other_ref, s_ref = refs[:4]
    p_ref, x_ref, w_ref, a_ref, b_ref, d_ref, g_ref, r_ref, sem = refs[4 + 2 * count :]
    n, own = a_ref.shape[0], p_ref.shape[0]
    half = own // 2
    band, core = where_ref[0], where_ref[1]

    copies = []
    for i, piece in enumerate(pieces):
        to = lax.rem(band + i // 2, count) * own + (i % 2) * half
        to = pl.multiple_of(to, 2 * SUB)
        copies.append(pltpu.make_async_copy(piece, w_ref.at[pl.ds(to, half), :], sem.at[i]))
        copies[-1].start()

    far = count // 2
    used = (far + 1) * own
    lane = lax.broadcasted_iota(jnp.int32, (half, mine_ref.shape[2]), 1)
    pad = jnp.zeros((half, n - mine_ref.shape[2]), jnp.float32)
    for x in range(count):
        for h in range(2):
            mine, other = mine_ref[x].astype(jnp.float32), other_ref[x].astype(jnp.float32)
            rows = jnp.where(core == h, mine, other)
            rows = jnp.concatenate([jnp.where(lane < used, rows, 0.0), pad], axis=1)
            shift = ((x - far) * own) % n
            if shift:
                rows = pltpu.roll(rows, shift, 1)
            at = x * own + h * half
            b_ref[at : at + half, :] = rows
    for i in range(0, n, BLK):
        for j in range(0, n, BLK):
            a_ref[i : i + BLK, j : j + BLK] = (
                b_ref[i : i + BLK, j : j + BLK] + b_ref[j : j + BLK, i : i + BLK].T
            )

    eliminate(a_ref, d_ref, g_ref, r_ref)

    row = lax.broadcasted_iota(jnp.int32, (n, n), 0)
    col = lax.broadcasted_iota(jnp.int32, (n, n), 1)
    a_ref[...] = jnp.where(row >= col, a_ref[...], 0.0)
    inverse = split(a_ref[...])
    overlap = pltpu.roll(s_ref[...], lax.rem(band + far, count) * own, 1)
    coupling = dot3(split(overlap), inverse, ((1,), (1,)))
    applied = -dot3(split(coupling), inverse, ((1,), (0,)))
    own_rows = a_ref[pl.ds(pl.multiple_of(band * own, SUB), own), :]
    hi, lo = split(jnp.concatenate([own_rows, applied], axis=0))
    both = jnp.concatenate([hi, lo], axis=0)

    for copy in copies:
        copy.wait()
    rows = hi.shape[0]
    for at in range(0, w_ref.shape[1], TILE):
        out = jnp.dot(both, w_ref[:, at : at + TILE], preferred_element_type=jnp.float32)
        out = (out[:rows] + out[rows:]).astype(jnp.bfloat16)
        p_ref[:, at : at + TILE] = out[:own]
        x_ref[:, at : at + TILE] = out[own:]


def project(where, mine, other, overlap, pieces, own):
    count = mine.shape[0]
    n, cols = count * own, pieces[0].shape[1]
    vmem = pl.BlockSpec(memory_space=pltpu.VMEM)
    return pl.pallas_call(
        functools.partial(project_kernel, count),
        out_shape=[
            jax.ShapeDtypeStruct((own, cols), jnp.bfloat16),
            jax.ShapeDtypeStruct((overlap.shape[0], cols), jnp.bfloat16),
        ],
        in_specs=[pl.BlockSpec(memory_space=pltpu.SMEM), vmem, vmem, vmem]
        + [pl.BlockSpec(memory_space=pl.ANY)] * len(pieces),
        out_specs=[vmem, vmem],
        scratch_shapes=[
            pltpu.VMEM((n, cols), jnp.bfloat16),
            pltpu.VMEM((n, n), jnp.float32),
            pltpu.VMEM((n, n), jnp.float32),
            pltpu.VMEM((BLK, BLK), jnp.float32),
            pltpu.VMEM((BLK, BLK), jnp.float32),
            pltpu.VMEM((BLK, n), jnp.float32),
            pltpu.SemaphoreType.DMA((len(pieces),)),
        ],
        name="project",
    )(where, mine, other, overlap, *pieces)


def ring(shard, left):
    count = lax.axis_size("band")
    ways = {s: [(i, (i + s) % count) for i in range(count)] for s in (1, -1)}
    mid = shard.shape[0] // 2
    halves = [shard[:mid], shard[mid:]]
    far = count // 2

    def dot(piece):
        return lax.dot_general(
            left, piece, (((1,), (1,)), ((), ())), preferred_element_type=jnp.float32
        )

    got, parts = {(0, h): halves[h] for h in range(2)}, {}
    moving = {(way, h): halves[h] for way, h in ((1, 0), (-1, 1), (1, 1), (-1, 0))}
    fresh = list(got)
    for s in range(1, far + 1):
        if s == far:
            moving = {key: moving[key] for key in ((1, 0), (-1, 1))}
        moving = {(way, h): lax.ppermute(x, "band", ways[way]) for (way, h), x in moving.items()}
        parts.update({key: dot(got[key]) for key in fresh})
        fresh = [(-way * s % count, h) for way, h in moving]
        got.update(zip(fresh, moving.values()))
    parts.update({key: dot(got[key]) for key in fresh})
    return got, parts


def to_all(shard, axis):
    count = lax.axis_size(axis)
    return lax.all_to_all(
        jnp.broadcast_to(shard[None], (count, *shard.shape)), axis, 0, 0, tiled=True
    )


def shards(orbitals, kernel, block_vectors):
    band, core, count = lax.axis_index("band"), lax.axis_index("core"), lax.axis_size("band")
    total = orbitals.shape[1] * lax.axis_size("y") * lax.axis_size("core")
    own, mine = orbitals.shape[0], block_vectors.shape[0]
    ho, hb = own // 2, mine // 2
    far = count // 2
    swap = [(0, 1), (1, 0)]

    weighted = (-(orbitals.astype(jnp.float32) * kernel[None, :])).astype(jnp.bfloat16)
    left = jnp.concatenate(
        [orbitals[:ho], block_vectors[:hb], orbitals[ho:], block_vectors[hb:]], axis=0
    )
    got, parts = ring(weighted, left)

    order = [((far + i) % count, h) for i in range(count) for h in range(2)]
    partial = jnp.concatenate([parts[key] for key in order], axis=1)
    n = own * count
    rows = ho + hb
    kept = lax.dynamic_slice_in_dim(partial, core * rows, rows, 0)
    sent = lax.dynamic_slice_in_dim(partial, (1 - core) * rows, rows, 0)
    kept = kept + lax.ppermute(sent, "core", swap)

    used = -(-(far + 1) * own // BLK) * BLK
    fold = ho // hb
    cols = n // fold
    packed = jnp.concatenate(
        [
            kept[:ho, :used],
            jnp.concatenate([kept[ho:, i * cols : (i + 1) * cols] for i in range(fold)], axis=0),
        ],
        axis=1,
    )
    summed = to_all(packed.astype(jnp.bfloat16), "y").astype(jnp.float32).sum(axis=0) / total
    column = lax.broadcasted_iota(jnp.int32, (ho, used), 1)
    twice = (column < own) | ((column >= far * own) & (column < (far + 1) * own))
    half_margin = -summed[:, :used] * jnp.where(twice, 0.5, 1.0)
    margin = to_all(half_margin.astype(jnp.bfloat16), "band")
    other_margin = lax.ppermute(margin, "core", swap)
    overlap = jnp.concatenate(
        [summed[i * hb : (i + 1) * hb, used:] for i in range(fold)], axis=1
    )
    other = lax.ppermute(overlap, "core", swap)
    overlap = jnp.where(
        core == 0,
        jnp.concatenate([overlap, other], axis=0),
        jnp.concatenate([other, overlap], axis=0),
    )
    where = jnp.stack([band, core]).astype(jnp.int32)
    pieces = [got[i, h] for i in range(count) for h in range(2)]
    return tuple(project(where, margin, other_margin, overlap, pieces, own))


def solution(mesh):
    images, ga, bands = (mesh.shape[a] for a in ("img", "ga", "band"))
    split_mesh = Mesh(
        mesh.devices.reshape(images, ga // 2, 2, bands), ("img", "y", "core", "band")
    )
    rows, cols = ("img", "band"), ("y", "core")
    return jax.shard_map(
        shards,
        mesh=split_mesh,
        in_specs=(P(rows, cols), P(cols), P(rows, cols)),
        out_specs=(P(rows, cols), P(rows, cols)),
        check_vma=False,
    )
```

```python
import functools

import jax
import jax.numpy as jnp
from jax import lax
from jax.experimental import pallas as pl
from jax.experimental.pallas import tpu as pltpu
from jax.sharding import Mesh
from jax.sharding import PartitionSpec as P

SUB = 8
BLK = 128
TILE = 512


def split(a):
    hi = a.astype(jnp.bfloat16)
    return hi, (a - hi.astype(jnp.float32)).astype(jnp.bfloat16)


def dot3(a, b, dims):
    (ah, al), (bh, bl) = a, b
    dot = functools.partial(
        lax.dot_general, dimension_numbers=(dims, ((), ())), preferred_element_type=jnp.float32
    )
    return dot(ah, bh) + (dot(ah, bl) + dot(al, bh))


def wide(x):
    return jnp.broadcast_to(x, (SUB, BLK))


def lanes(x, k):
    return [wide(x[:, k + j : k + j + 1]) for j in range(SUB)]


def total_of(terms):
    while len(terms) > 1:
        odd = [terms[-1]] if len(terms) % 2 else []
        terms = [a + b for a, b in zip(terms[::2], terms[1::2])] + odd
    return terms[0]


def inverse_of_factor(rows, inv):
    sub = lax.broadcasted_iota(jnp.int32, (SUB, BLK), 0)
    at = [sub == j for j in range(SUB)]
    cols = lanes(rows[0], 0)
    for p in range(len(rows)):
        k = p * SUB
        v, g = rows[p], inv[p]
        last = p + 1 == len(rows)
        if not last:
            ahead, below = lanes(rows[p + 1], k + SUB), lanes(rows[p + 1], k)
        out, unit, recips = g, {}, []
        for j in range(SUB):
            pivot, cj = wide(cols[j][j : j + 1]), cols[j]
            recip = 1.0 / pivot
            recips.append(recip)
            for m in range(j + 1, SUB):
                t = wide(cols[m][j : j + 1]) * recip
                unit[j, m] = t
                cols[m] = jnp.where(at[j], t, cols[m] - cj * t)
            gj = wide(g[j : j + 1])
            out = jnp.where(at[j], gj * lax.rsqrt(pivot), out)
            vj, gj = wide(v[j : j + 1]) * recip, gj * recip
            v = jnp.where(at[j], vj, v - cj * vj)
            g = jnp.where(at[j], gj, g - cj * gj)
        inv[p] = out
        if last:
            break
        lower = list(below)
        for j in range(SUB):
            for m in range(j + 1, SUB):
                lower[m] = lower[m] - lower[j] * unit[j, m]
        scaled = [lower[j] * recips[j] for j in range(SUB)]
        cols = [
            ahead[m] - total_of([lower[j] * wide(scaled[j][m : m + 1]) for j in range(SUB)])
            for m in range(SUB)
        ]
        vs = [wide(v[j : j + 1]) for j in range(SUB)]
        gs = [wide(g[j : j + 1]) for j in range(SUB)]
        for q in range(p + 1, len(rows)):
            c = below if q == p + 1 else lanes(rows[q], k)
            rows[q] = rows[q] - total_of([c[j] * vs[j] for j in range(SUB)])
            inv[q] = inv[q] - total_of([c[j] * gs[j] for j in range(SUB)])
    return inv


def eliminate(a, d_ref, g_ref, r_ref):
    blocks = a.shape[0] // BLK
    row = lax.broadcasted_iota(jnp.int32, (SUB, BLK), 0)
    col = lax.broadcasted_iota(jnp.int32, (SUB, BLK), 1)
    groups = range(BLK // SUB)
    rows_of = ((0,), (0,))

    def block(i):
        return pl.ds(pl.multiple_of(i * BLK, BLK), BLK)

    d_ref[...] = a[:BLK, :BLK]
    r_ref[...] = jnp.zeros(r_ref.shape, jnp.float32)

    def step(b, _):
        rows = [d_ref[SUB * i : SUB * (i + 1), :] for i in groups]
        inv = [jnp.where(col == row + SUB * i, 1.0, 0.0) for i in groups]
        for i, g in enumerate(inverse_of_factor(rows, inv)):
            g_ref[SUB * i : SUB * (i + 1), :] = g
        r = split(r_ref[...])
        before = block(lax.rem(b + blocks - 1, blocks))
        for i in range(blocks - 1):
            them = block(lax.rem(b + i, blocks))
            live = jnp.logical_and(b > 0, b + i < blocks)
            factor = jnp.where(live, r_ref[:, them], 0.0)
            a[them, before] = jnp.where(live, 0.0, a[them, before])
            a[them, :] = a[them, :] - dot3(split(factor), r, rows_of)
        here, after = block(b), block(jnp.minimum(b + 1, blocks - 1))
        g = g_ref[...]
        r_ref[...] = dot3(split(g), split(a[here, :]), ((1,), (0,)))
        factor = split(r_ref[:, after])
        d_ref[...] = a[after, after] - dot3(factor, factor, rows_of)
        r_ref[:, here] = g
        a[here, :] = r_ref[...]
        return 0

    lax.fori_loop(0, blocks, step, 0)


def project_kernel(count, *refs):
    pieces = refs[6 : 6 + 2 * count]
    band_ref, core_ref, mine_ref, other_ref, s_ref, s_other_ref = refs[:6]
    p_ref, x_ref, w_ref, a_ref, b_ref, d_ref, g_ref, r_ref, sem = refs[6 + 2 * count :]
    n, own = a_ref.shape[0], p_ref.shape[0]
    half = own // 2
    band, core = band_ref[0], core_ref[0]

    copies = []
    for i, piece in enumerate(pieces):
        to = lax.rem(band + i // 2, count) * own + (i % 2) * half
        to = pl.multiple_of(to, 2 * SUB)
        copies.append(pltpu.make_async_copy(piece, w_ref.at[pl.ds(to, half), :], sem.at[i]))
        copies[-1].start()

    far = count // 2
    used = (far + 1) * own
    lane = lax.broadcasted_iota(jnp.int32, (half, mine_ref.shape[2]), 1)
    pad = jnp.zeros((half, n - mine_ref.shape[2]), jnp.float32)
    for x in range(count):
        for h in range(2):
            mine, other = mine_ref[x].astype(jnp.float32), other_ref[x].astype(jnp.float32)
            rows = jnp.where(core == h, mine, other)
            rows = jnp.concatenate([jnp.where(lane < used, rows, 0.0), pad], axis=1)
            shift = ((x - far) * own) % n
            if shift:
                rows = pltpu.roll(rows, shift, 1)
            at = x * own + h * half
            b_ref[at : at + half, :] = rows
    for i in range(0, n, BLK):
        for j in range(0, n, BLK):
            a_ref[i : i + BLK, j : j + BLK] = (
                b_ref[i : i + BLK, j : j + BLK] + b_ref[j : j + BLK, i : i + BLK].T
            )

    eliminate(a_ref, d_ref, g_ref, r_ref)

    row = lax.broadcasted_iota(jnp.int32, (n, n), 0)
    col = lax.broadcasted_iota(jnp.int32, (n, n), 1)
    a_ref[...] = jnp.where(row >= col, a_ref[...], 0.0)
    inverse = split(a_ref[...])
    overlap = jnp.concatenate(
        [
            jnp.where(core == 0, s_ref[...], s_other_ref[...]),
            jnp.where(core == 0, s_other_ref[...], s_ref[...]),
        ],
        axis=0,
    )
    overlap = pltpu.roll(overlap, lax.rem(band + far, count) * own, 1)
    coupling = dot3(split(overlap), inverse, ((1,), (1,)))
    applied = -dot3(split(coupling), inverse, ((1,), (0,)))
    own_rows = a_ref[pl.ds(pl.multiple_of(band * own, SUB), own), :]
    hi, lo = split(jnp.concatenate([own_rows, applied], axis=0))
    both = jnp.concatenate([hi, lo], axis=0)

    for copy in copies:
        copy.wait()
    rows = hi.shape[0]
    for at in range(0, w_ref.shape[1], TILE):
        out = jnp.dot(both, w_ref[:, at : at + TILE], preferred_element_type=jnp.float32)
        out = (out[:rows] + out[rows:]).astype(jnp.bfloat16)
        p_ref[:, at : at + TILE] = out[:own]
        x_ref[:, at : at + TILE] = out[own:]


def project(band, core, mine, other, overlap, other_overlap, pieces, own):
    count = mine.shape[0]
    n, cols = count * own, pieces[0].shape[1]
    vmem = pl.BlockSpec(memory_space=pltpu.VMEM)
    return pl.pallas_call(
        functools.partial(project_kernel, count),
        out_shape=[
            jax.ShapeDtypeStruct((own, cols), jnp.bfloat16),
            jax.ShapeDtypeStruct((2 * overlap.shape[0], cols), jnp.bfloat16),
        ],
        in_specs=[pl.BlockSpec(memory_space=pltpu.SMEM)] * 2
        + [vmem] * 4
        + [pl.BlockSpec(memory_space=pl.ANY)] * len(pieces),
        out_specs=[vmem, vmem],
        scratch_shapes=[
            pltpu.VMEM((n, cols), jnp.bfloat16),
            pltpu.VMEM((n, n), jnp.float32),
            pltpu.VMEM((n, n), jnp.float32),
            pltpu.VMEM((BLK, BLK), jnp.float32),
            pltpu.VMEM((BLK, BLK), jnp.float32),
            pltpu.VMEM((BLK, n), jnp.float32),
            pltpu.SemaphoreType.DMA((len(pieces),)),
        ],
        name="project",
    )(band[None], core[None], mine, other, overlap, other_overlap, *pieces)


def ring(shard, left):
    count = lax.axis_size("band")
    ways = {s: [(i, (i + s) % count) for i in range(count)] for s in (1, -1)}
    mid = shard.shape[0] // 2
    halves = [shard[:mid], shard[mid:]]
    far = count // 2

    def dot(piece):
        return lax.dot_general(
            left, piece, (((1,), (1,)), ((), ())), preferred_element_type=jnp.float32
        )

    got, parts = {(0, h): halves[h] for h in range(2)}, {}
    moving = {(way, h): halves[h] for way, h in ((1, 0), (-1, 1), (1, 1), (-1, 0))}
    fresh = list(got)
    for s in range(1, far + 1):
        if s == far:
            moving = {key: moving[key] for key in ((1, 0), (-1, 1))}
        for way, h in list(moving):
            x, before = moving[way, h], (-way * (s - 2) % count, h)
            if s > 1:
                x, parts[before] = lax.optimization_barrier((x, parts[before]))
            moving[way, h] = lax.ppermute(x, "band", ways[way])
        parts.update({key: dot(got[key]) for key in fresh})
        fresh = [(-way * s % count, h) for way, h in moving]
        got.update(zip(fresh, moving.values()))
    parts.update({key: dot(got[key]) for key in fresh})
    return got, parts


def to_all(shard, axis):
    count = lax.axis_size(axis)
    return lax.all_to_all(
        jnp.broadcast_to(shard[None], (count, *shard.shape)), axis, 0, 0, tiled=True
    )


def shards(orbitals, kernel, block_vectors):
    band, core, count = lax.axis_index("band"), lax.axis_index("core"), lax.axis_size("band")
    total = orbitals.shape[1] * lax.axis_size("y") * lax.axis_size("core")
    own, mine = orbitals.shape[0], block_vectors.shape[0]
    ho, hb = own // 2, mine // 2
    far = count // 2
    swap = [(0, 1), (1, 0)]

    weighted = (-(orbitals.astype(jnp.float32) * kernel[None, :])).astype(jnp.bfloat16)
    left = jnp.concatenate(
        [orbitals[:ho], block_vectors[:hb], orbitals[ho:], block_vectors[hb:]], axis=0
    )
    got, parts = ring(weighted, left)

    order = [((far + i) % count, h) for i in range(count) for h in range(2)]
    partial = jnp.concatenate([parts[key] for key in order], axis=1)
    n = own * count
    rows = ho + hb
    kept = lax.dynamic_slice_in_dim(partial, core * rows, rows, 0)
    sent = lax.dynamic_slice_in_dim(partial, (1 - core) * rows, rows, 0)
    kept = kept + lax.ppermute(sent, "core", swap)

    used = -(-(far + 1) * own // BLK) * BLK
    fold = ho // hb
    cols = n // fold
    packed = jnp.concatenate(
        [
            kept[:ho, :used],
            jnp.concatenate([kept[ho:, i * cols : (i + 1) * cols] for i in range(fold)], axis=0),
        ],
        axis=1,
    )
    summed = to_all(packed.astype(jnp.bfloat16), "y").astype(jnp.float32).sum(axis=0) / total
    column = lax.broadcasted_iota(jnp.int32, (ho, used), 1)
    twice = (column < own) | ((column >= far * own) & (column < (far + 1) * own))
    half_margin = -summed[:, :used] * jnp.where(twice, 0.5, 1.0)
    margin = to_all(half_margin.astype(jnp.bfloat16), "band")
    other_margin = lax.ppermute(margin, "core", swap)
    overlap = jnp.concatenate(
        [summed[i * hb : (i + 1) * hb, used:] for i in range(fold)], axis=1
    )
    other = lax.ppermute(overlap, "core", swap)
    pieces = [got[i, h] for i in range(count) for h in range(2)]
    return tuple(project(band, core, margin, other_margin, overlap, other, pieces, own))


def solution(mesh):
    images, ga, bands = (mesh.shape[a] for a in ("img", "ga", "band"))
    split_mesh = Mesh(
        mesh.devices.reshape(images, ga // 2, 2, bands), ("img", "y", "core", "band")
    )
    rows, cols = ("img", "band"), ("y", "core")
    return jax.shard_map(
        shards,
        mesh=split_mesh,
        in_specs=(P(rows, cols), P(cols), P(rows, cols)),
        out_specs=(P(rows, cols), P(rows, cols)),
        check_vma=False,
    )
```

```python
import functools

import jax
import jax.numpy as jnp
from jax import lax
from jax.experimental import pallas as pl
from jax.experimental.pallas import tpu as pltpu
from jax.sharding import Mesh
from jax.sharding import PartitionSpec as P

SUB = 8
BLK = 128
TILE = 512
NEAR = 2


def split(a):
    hi = a.astype(jnp.bfloat16)
    return hi, (a - hi.astype(jnp.float32)).astype(jnp.bfloat16)


def dot3(a, b, dims):
    (ah, al), (bh, bl) = a, b
    dot = functools.partial(
        lax.dot_general, dimension_numbers=(dims, ((), ())), preferred_element_type=jnp.float32
    )
    return dot(ah, bh) + (dot(ah, bl) + dot(al, bh))


def wide(x):
    return jnp.broadcast_to(x, (SUB, BLK))


def lanes(x, k):
    return [wide(x[:, k + j : k + j + 1]) for j in range(SUB)]


def total_of(terms):
    while len(terms) > 1:
        odd = [terms[-1]] if len(terms) % 2 else []
        terms = [a + b for a, b in zip(terms[::2], terms[1::2])] + odd
    return terms[0]


def around(x, before, after):
    parts = [jnp.zeros((before, x.shape[1]), x.dtype), x, jnp.zeros((after, x.shape[1]), x.dtype)]
    return jnp.concatenate([part for part in parts if part.shape[0]], axis=0)


def inverse_of_factor(rows, inv):
    sub = lax.broadcasted_iota(jnp.int32, (SUB, BLK), 0)
    at = [sub == j for j in range(SUB)]
    cols = lanes(rows[0], 0)
    for p in range(len(rows)):
        k = p * SUB
        v, g = rows[p], inv[p]
        last = p + 1 == len(rows)
        if not last:
            ahead, below = lanes(rows[p + 1], k + SUB), lanes(rows[p + 1], k)
        out, unit, recips = g, {}, []
        for j in range(SUB):
            pivot, cj = wide(cols[j][j : j + 1]), cols[j]
            recip = 1.0 / pivot
            recips.append(recip)
            for m in range(j + 1, SUB):
                t = wide(cols[m][j : j + 1]) * recip
                unit[j, m] = t
                cols[m] = jnp.where(at[j], t, cols[m] - cj * t)
            gj = wide(g[j : j + 1])
            out = jnp.where(at[j], gj * lax.rsqrt(pivot), out)
            vj, gj = wide(v[j : j + 1]) * recip, gj * recip
            v = jnp.where(at[j], vj, v - cj * vj)
            g = jnp.where(at[j], gj, g - cj * gj)
        inv[p] = out
        if last:
            break
        lower = list(below)
        for j in range(SUB):
            for m in range(j + 1, SUB):
                lower[m] = lower[m] - lower[j] * unit[j, m]
        scaled = [lower[j] * recips[j] for j in range(SUB)]
        cols = [
            ahead[m] - total_of([lower[j] * wide(scaled[j][m : m + 1]) for j in range(SUB)])
            for m in range(SUB)
        ]
        far = min(p + 1 + NEAR, len(rows))
        if far < len(rows):
            pivots = jnp.concatenate([v, g], axis=1)
            zeros = jnp.zeros_like(pivots)
            pivots = [zeros, pivots] if p % 2 else [pivots, zeros]
            pivots = split(jnp.concatenate(pivots, axis=0))
            first = p // 2 * 2 * SUB
            pivots = [around(x, first, BLK - first - 2 * SUB) for x in pivots]
            taken = dot3(split(jnp.concatenate(rows[far:], axis=0)), pivots, ((1,), (0,)))
        vs = [wide(v[j : j + 1]) for j in range(SUB)]
        gs = [wide(g[j : j + 1]) for j in range(SUB)]
        for q in range(p + 1, len(rows)):
            if q < far:
                c = below if q == p + 1 else lanes(rows[q], k)
                rows[q] = rows[q] - total_of([c[j] * vs[j] for j in range(SUB)])
                inv[q] = inv[q] - total_of([c[j] * gs[j] for j in range(SUB)])
            else:
                i = (q - far) * SUB
                rows[q] = rows[q] - taken[i : i + SUB, :BLK]
                inv[q] = inv[q] - taken[i : i + SUB, BLK:]
    return inv


def eliminate(a, d_ref, g_ref, r_ref):
    blocks = a.shape[0] // BLK
    row = lax.broadcasted_iota(jnp.int32, (SUB, BLK), 0)
    col = lax.broadcasted_iota(jnp.int32, (SUB, BLK), 1)
    groups = range(BLK // SUB)
    rows_of = ((0,), (0,))

    def block(i):
        return pl.ds(pl.multiple_of(i * BLK, BLK), BLK)

    d_ref[...] = a[:BLK, :BLK]
    r_ref[...] = jnp.zeros(r_ref.shape, jnp.float32)

    def step(b, _):
        rows = [d_ref[SUB * i : SUB * (i + 1), :] for i in groups]
        inv = [jnp.where(col == row + SUB * i, 1.0, 0.0) for i in groups]
        for i, g in enumerate(inverse_of_factor(rows, inv)):
            g_ref[SUB * i : SUB * (i + 1), :] = g
        r = split(r_ref[...])
        before = block(lax.rem(b + blocks - 1, blocks))
        for i in range(blocks - 1):
            them = block(lax.rem(b + i, blocks))
            live = jnp.logical_and(b > 0, b + i < blocks)
            factor = jnp.where(live, r_ref[:, them], 0.0)
            a[them, before] = jnp.where(live, 0.0, a[them, before])
            a[them, :] = a[them, :] - dot3(split(factor), r, rows_of)
        here, after = block(b), block(jnp.minimum(b + 1, blocks - 1))
        g = g_ref[...]
        r_ref[...] = dot3(split(g), split(a[here, :]), ((1,), (0,)))
        factor = split(r_ref[:, after])
        d_ref[...] = a[after, after] - dot3(factor, factor, rows_of)
        r_ref[:, here] = g
        a[here, :] = r_ref[...]
        return 0

    lax.fori_loop(0, blocks, step, 0)


def project_kernel(count, *refs):
    pieces = refs[6 : 6 + 2 * count]
    band_ref, core_ref, mine_ref, other_ref, s_ref, s_other_ref = refs[:6]
    p_ref, x_ref, w_ref, a_ref, b_ref, d_ref, g_ref, r_ref, sem = refs[6 + 2 * count :]
    n, own = a_ref.shape[0], p_ref.shape[0]
    half = own // 2
    band, core = band_ref[0], core_ref[0]

    copies = []
    for i, piece in enumerate(pieces):
        to = lax.rem(band + i // 2, count) * own + (i % 2) * half
        to = pl.multiple_of(to, 2 * SUB)
        copies.append(pltpu.make_async_copy(piece, w_ref.at[pl.ds(to, half), :], sem.at[i]))
        copies[-1].start()

    far = count // 2
    used = (far + 1) * own
    lane = lax.broadcasted_iota(jnp.int32, (half, mine_ref.shape[2]), 1)
    twice = (lane < own) | (lane >= far * own)
    weight = jnp.where(lane < used, jnp.where(twice, 0.5, 1.0), 0.0)
    pad = jnp.zeros((half, n - mine_ref.shape[2]), jnp.float32)
    for x in range(count):
        for h in range(2):
            mine, other = mine_ref[x].astype(jnp.float32), other_ref[x].astype(jnp.float32)
            rows = jnp.where(core == h, mine, other)
            rows = jnp.where(lane < used, rows, 0.0) * weight
            rows = jnp.concatenate([rows, pad], axis=1)
            shift = ((x - far) * own) % n
            if shift:
                rows = pltpu.roll(rows, shift, 1)
            at = x * own + h * half
            b_ref[at : at + half, :] = rows
    for i in range(0, n, BLK):
        for j in range(0, n, BLK):
            a_ref[i : i + BLK, j : j + BLK] = (
                b_ref[i : i + BLK, j : j + BLK] + b_ref[j : j + BLK, i : i + BLK].T
            )

    eliminate(a_ref, d_ref, g_ref, r_ref)

    row = lax.broadcasted_iota(jnp.int32, (n, n), 0)
    col = lax.broadcasted_iota(jnp.int32, (n, n), 1)
    a_ref[...] = jnp.where(row >= col, a_ref[...], 0.0)
    inverse = split(a_ref[...])
    overlap = jnp.concatenate(
        [
            jnp.where(core == 0, s_ref[...], s_other_ref[...]),
            jnp.where(core == 0, s_other_ref[...], s_ref[...]),
        ],
        axis=0,
    )
    overlap = pltpu.roll(overlap, lax.rem(band + far, count) * own, 1)
    coupling = dot3(split(overlap), inverse, ((1,), (1,)))
    applied = -dot3(split(coupling), inverse, ((1,), (0,)))
    own_rows = a_ref[pl.ds(pl.multiple_of(band * own, SUB), own), :]
    coefs = jnp.concatenate([own_rows, applied], axis=0).astype(jnp.bfloat16)

    for copy in copies:
        copy.wait()
    for at in range(0, w_ref.shape[1], TILE):
        out = jnp.dot(coefs, w_ref[:, at : at + TILE], preferred_element_type=jnp.float32)
        out = out.astype(jnp.bfloat16)
        p_ref[:, at : at + TILE] = out[:own]
        x_ref[:, at : at + TILE] = out[own:]


def project(band, core, mine, other, overlap, other_overlap, pieces, own):
    count = mine.shape[0]
    n, cols = count * own, pieces[0].shape[1]
    vmem = pl.BlockSpec(memory_space=pltpu.VMEM)
    return pl.pallas_call(
        functools.partial(project_kernel, count),
        out_shape=[
            jax.ShapeDtypeStruct((own, cols), jnp.bfloat16),
            jax.ShapeDtypeStruct((2 * overlap.shape[0], cols), jnp.bfloat16),
        ],
        in_specs=[pl.BlockSpec(memory_space=pltpu.SMEM)] * 2
        + [vmem] * 4
        + [pl.BlockSpec(memory_space=pl.ANY)] * len(pieces),
        out_specs=[vmem, vmem],
        scratch_shapes=[
            pltpu.VMEM((n, cols), jnp.bfloat16),
            pltpu.VMEM((n, n), jnp.float32),
            pltpu.VMEM((n, n), jnp.float32),
            pltpu.VMEM((BLK, BLK), jnp.float32),
            pltpu.VMEM((BLK, BLK), jnp.float32),
            pltpu.VMEM((BLK, n), jnp.float32),
            pltpu.SemaphoreType.DMA((len(pieces),)),
        ],
        name="project",
    )(band[None], core[None], mine, other, overlap, other_overlap, *pieces)


def ring(shard, left):
    count = lax.axis_size("band")
    ways = {s: [(i, (i + s) % count) for i in range(count)] for s in (1, -1)}
    mid = shard.shape[0] // 2
    halves = [shard[:mid], shard[mid:]]
    far = count // 2

    def dot(piece):
        return lax.dot_general(
            left, piece, (((1,), (1,)), ((), ())), preferred_element_type=jnp.float32
        )

    longer = ((1, 0), (-1, 1))
    got = {(0, h): halves[h] for h in range(2)}
    parts = {key: dot(x) for key, x in got.items()}
    moving = {(way, h): halves[h] for way, h in longer + ((1, 1), (-1, 0))}
    for s in range(1, far + 1):
        fresh = {}
        for (way, h), x in moving.items():
            long = (way, h) in longer
            if s == far and not long:
                continue
            before = (-way * (s - 2) % count, h) if s > 1 else (0, h)
            if s > 1 or not long:
                x, parts[before] = lax.optimization_barrier((x, parts[before]))
            fresh[way, h] = lax.ppermute(x, "band", ways[way])
        if s > 1:
            for way, h in moving:
                key = (-way * (s - 1) % count, h)
                parts[key] = dot(got[key])
        moving = fresh
        got.update({(-way * s % count, h): x for (way, h), x in moving.items()})
    for way, h in moving:
        key = (-way * far % count, h)
        parts[key] = dot(got[key])
    return got, parts


def to_all(shard, axis):
    count = lax.axis_size(axis)
    return lax.all_to_all(
        jnp.broadcast_to(shard[None], (count, *shard.shape)), axis, 0, 0, tiled=True
    )


def shards(orbitals, kernel, block_vectors):
    band, core, count = lax.axis_index("band"), lax.axis_index("core"), lax.axis_size("band")
    total = orbitals.shape[1] * lax.axis_size("y") * lax.axis_size("core")
    own, mine = orbitals.shape[0], block_vectors.shape[0]
    ho, hb = own // 2, mine // 2
    far = count // 2
    swap = [(0, 1), (1, 0)]

    weighted = (-(orbitals.astype(jnp.float32) * kernel[None, :])).astype(jnp.bfloat16)
    left = jnp.concatenate(
        [orbitals[:ho], block_vectors[:hb], orbitals[ho:], block_vectors[hb:]], axis=0
    )
    got, parts = ring(weighted, left)

    order = [((far + i) % count, h) for i in range(count) for h in range(2)]
    partial = jnp.concatenate([parts[key] for key in order], axis=1)
    n = own * count
    rows = ho + hb
    kept = lax.dynamic_slice_in_dim(partial, core * rows, rows, 0)
    sent = lax.dynamic_slice_in_dim(partial, (1 - core) * rows, rows, 0)
    kept = kept + lax.ppermute(sent, "core", swap)

    used = -(-(far + 1) * own // BLK) * BLK
    fold = ho // hb
    cols = n // fold
    packed = jnp.concatenate(
        [
            kept[:ho, :used],
            jnp.concatenate([kept[ho:, i * cols : (i + 1) * cols] for i in range(fold)], axis=0),
        ],
        axis=1,
    )
    summed = to_all(packed.astype(jnp.bfloat16), "y").astype(jnp.float32).sum(axis=0) / total
    margin = to_all((-summed[:, :used]).astype(jnp.bfloat16), "band")
    other_margin = lax.ppermute(margin, "core", swap)
    overlap = jnp.concatenate(
        [summed[i * hb : (i + 1) * hb, used:] for i in range(fold)], axis=1
    )
    other = lax.ppermute(overlap, "core", swap)
    pieces = [got[i, h] for i in range(count) for h in range(2)]
    return tuple(project(band, core, margin, other_margin, overlap, other, pieces, own))


def solution(mesh):
    images, ga, bands = (mesh.shape[a] for a in ("img", "ga", "band"))
    split_mesh = Mesh(
        mesh.devices.reshape(images, ga // 2, 2, bands), ("img", "y", "core", "band")
    )
    rows, cols = ("img", "band"), ("y", "core")
    return jax.shard_map(
        shards,
        mesh=split_mesh,
        in_specs=(P(rows, cols), P(cols), P(rows, cols)),
        out_specs=(P(rows, cols), P(rows, cols)),
        check_vma=False,
    )
```

```python
import functools

import jax
import jax.numpy as jnp
from jax import lax
from jax.experimental import pallas as pl
from jax.experimental.pallas import tpu as pltpu
from jax.sharding import Mesh
from jax.sharding import PartitionSpec as P


SUB = 8
BLK = 128
TILE = 512
NEAR = 2


def split(a):
    hi = a.astype(jnp.bfloat16)
    return hi, (a - hi.astype(jnp.float32)).astype(jnp.bfloat16)


def dot3(a, b, dims):
    (ah, al), (bh, bl) = a, b
    dot = functools.partial(
        lax.dot_general, dimension_numbers=(dims, ((), ())), preferred_element_type=jnp.float32
    )
    return dot(ah, bh) + (dot(ah, bl) + dot(al, bh))


def dot1(a, b, dims):
    a, b = a.astype(jnp.bfloat16), b.astype(jnp.bfloat16)
    return lax.dot_general(a, b, (dims, ((), ())), preferred_element_type=jnp.float32)


def dot2(a, b, dims):
    both = dot1(jnp.concatenate(split(a), axis=0), b, dims)
    return both[: a.shape[0]] + both[a.shape[0] :]


def wide(x):
    return jnp.broadcast_to(x, (SUB, BLK))


def lanes(x, k):
    return [wide(x[:, k + j : k + j + 1]) for j in range(SUB)]


def total_of(terms):
    while len(terms) > 1:
        odd = [terms[-1]] if len(terms) % 2 else []
        terms = [a + b for a, b in zip(terms[::2], terms[1::2])] + odd
    return terms[0]


def around(x, before, after):
    parts = [jnp.zeros((before, x.shape[1]), x.dtype), x, jnp.zeros((after, x.shape[1]), x.dtype)]
    return jnp.concatenate([part for part in parts if part.shape[0]], axis=0)


def inverse_of_factor(rows, inv):
    sub = lax.broadcasted_iota(jnp.int32, (SUB, BLK), 0)
    at = [sub == j for j in range(SUB)]
    cols = lanes(rows[0], 0)
    for p in range(len(rows)):
        k = p * SUB
        v, g = rows[p], inv[p]
        last = p + 1 == len(rows)
        if not last:
            ahead, below = lanes(rows[p + 1], k + SUB), lanes(rows[p + 1], k)
        out, unit, recips = g, {}, []
        for j in range(SUB):
            pivot, cj = wide(cols[j][j : j + 1]), cols[j]
            recip = 1.0 / pivot
            recips.append(recip)
            for m in range(j + 1, SUB):
                t = wide(cols[m][j : j + 1]) * recip
                unit[j, m] = t
                cols[m] = jnp.where(at[j], t, cols[m] - cj * t)
            gj = wide(g[j : j + 1])
            out = jnp.where(at[j], gj * lax.rsqrt(pivot), out)
            vj, gj = wide(v[j : j + 1]) * recip, gj * recip
            v = jnp.where(at[j], vj, v - cj * vj)
            g = jnp.where(at[j], gj, g - cj * gj)
        inv[p] = out
        if last:
            break
        lower = list(below)
        for j in range(SUB):
            for m in range(j + 1, SUB):
                lower[m] = lower[m] - lower[j] * unit[j, m]
        scaled = [lower[j] * recips[j] for j in range(SUB)]
        cols = [
            ahead[m] - total_of([lower[j] * wide(scaled[j][m : m + 1]) for j in range(SUB)])
            for m in range(SUB)
        ]
        far = min(p + 1 + NEAR, len(rows))
        if far < len(rows):
            pivots = jnp.concatenate([v, g], axis=1)
            zeros = jnp.zeros_like(pivots)
            pivots = [zeros, pivots] if p % 2 else [pivots, zeros]
            first = p // 2 * 2 * SUB
            pivots = jnp.concatenate(pivots, axis=0).astype(jnp.bfloat16)
            pivots = around(pivots, first, BLK - first - 2 * SUB)
            taken = dot1(jnp.concatenate(rows[far:], axis=0), pivots, ((1,), (0,)))
        vs = [wide(v[j : j + 1]) for j in range(SUB)]
        gs = [wide(g[j : j + 1]) for j in range(SUB)]
        for q in range(p + 1, len(rows)):
            if q < far:
                c = below if q == p + 1 else lanes(rows[q], k)
                rows[q] = rows[q] - total_of([c[j] * vs[j] for j in range(SUB)])
                inv[q] = inv[q] - total_of([c[j] * gs[j] for j in range(SUB)])
            else:
                i = (q - far) * SUB
                rows[q] = rows[q] - taken[i : i + SUB, :BLK]
                inv[q] = inv[q] - taken[i : i + SUB, BLK:]
    return inv


def eliminate(a, d_ref, g_ref, r_ref):
    blocks = a.shape[0] // BLK
    row = lax.broadcasted_iota(jnp.int32, (SUB, BLK), 0)
    col = lax.broadcasted_iota(jnp.int32, (SUB, BLK), 1)
    groups = range(BLK // SUB)
    rows_of = ((0,), (0,))

    def block(i):
        return pl.ds(pl.multiple_of(i * BLK, BLK), BLK)

    d_ref[...] = a[:BLK, :BLK]
    r_ref[...] = jnp.zeros(r_ref.shape, jnp.float32)

    def step(b, _):
        rows = [d_ref[SUB * i : SUB * (i + 1), :] for i in groups]
        inv = [jnp.where(col == row + SUB * i, 1.0, 0.0) for i in groups]
        for i, g in enumerate(inverse_of_factor(rows, inv)):
            g_ref[SUB * i : SUB * (i + 1), :] = g
        r = r_ref[...].astype(jnp.bfloat16)
        before = block(lax.rem(b + blocks - 1, blocks))
        for i in range(blocks - 1):
            them = block(lax.rem(b + i, blocks))
            live = jnp.logical_and(b > 0, b + i < blocks)
            factor = jnp.where(live, r_ref[:, them], 0.0)
            a[them, before] = jnp.where(live, 0.0, a[them, before])
            a[them, :] = a[them, :] - dot1(factor, r, rows_of)
        here, after = block(b), block(jnp.minimum(b + 1, blocks - 1))
        g = g_ref[...]
        r_ref[...] = dot3(split(g), split(a[here, :]), ((1,), (0,)))
        factor = r_ref[:, after]
        d_ref[...] = a[after, after] - dot1(factor, factor, rows_of)
        r_ref[:, here] = g
        a[here, :] = r_ref[...]
        return 0

    lax.fori_loop(0, blocks, step, 0)


def project_kernel(count, keys, *refs):
    pieces = refs[6 : 6 + len(keys)]
    band_ref, core_ref, mine_ref, other_ref, s_ref, s_other_ref = refs[:6]
    p_ref, x_ref, w_ref, a_ref, b_ref, d_ref, g_ref, r_ref, sem = refs[6 + len(keys) :]
    n, own = a_ref.shape[0], p_ref.shape[0]
    half = own // 2
    band, core = band_ref[0], core_ref[0]

    copies = []
    for i, ((distance, first, rows), piece) in enumerate(zip(keys, pieces)):
        to = pl.multiple_of(lax.rem(band + distance, count) * own + first, SUB)
        copies.append(pltpu.make_async_copy(piece, w_ref.at[pl.ds(to, rows), :], sem.at[i]))
        copies[-1].start()

    far = count // 2
    used = (far + 1) * own
    lane = lax.broadcasted_iota(jnp.int32, (half, mine_ref.shape[2]), 1)
    twice = (lane < own) | (lane >= far * own)
    weight = jnp.where(lane < used, jnp.where(twice, 0.5, 1.0), 0.0)
    pad = jnp.zeros((half, n - mine_ref.shape[2]), jnp.float32)
    for x in range(count):
        for h in range(2):
            mine, other = mine_ref[x].astype(jnp.float32), other_ref[x].astype(jnp.float32)
            rows = jnp.where(core == h, mine, other)
            rows = jnp.where(lane < used, rows, 0.0) * weight
            rows = jnp.concatenate([rows, pad], axis=1)
            shift = ((x - far) * own) % n
            if shift:
                rows = pltpu.roll(rows, shift, 1)
            at = x * own + h * half
            b_ref[at : at + half, :] = rows
    for i in range(0, n, BLK):
        for j in range(0, n, BLK):
            a_ref[i : i + BLK, j : j + BLK] = (
                b_ref[i : i + BLK, j : j + BLK] + b_ref[j : j + BLK, i : i + BLK].T
            )

    eliminate(a_ref, d_ref, g_ref, r_ref)

    row = lax.broadcasted_iota(jnp.int32, (n, n), 0)
    col = lax.broadcasted_iota(jnp.int32, (n, n), 1)
    inverse = jnp.where(row >= col, a_ref[...], 0.0).astype(jnp.bfloat16)
    overlap = jnp.concatenate(
        [
            jnp.where(core == 0, s_ref[...], s_other_ref[...]),
            jnp.where(core == 0, s_other_ref[...], s_ref[...]),
        ],
        axis=0,
    )
    overlap = pltpu.roll(overlap, lax.rem(band + far, count) * own, 1)
    coupling = dot2(overlap, inverse, ((1,), (1,)))
    applied = -dot2(coupling, inverse, ((1,), (0,)))
    first = pl.multiple_of(band * own, SUB)
    own_row = first + lax.broadcasted_iota(jnp.int32, (own, n), 0)
    own_rows = jnp.where(own_row >= col[:own], a_ref[pl.ds(first, own), :], 0.0)
    coefs = jnp.concatenate([own_rows, applied], axis=0).astype(jnp.bfloat16)

    for copy in copies:
        copy.wait()
    for at in range(0, w_ref.shape[1], TILE):
        out = jnp.dot(coefs, w_ref[:, at : at + TILE], preferred_element_type=jnp.float32)
        out = out.astype(jnp.bfloat16)
        p_ref[:, at : at + TILE] = out[:own]
        x_ref[:, at : at + TILE] = out[own:]


def project(band, core, mine, other, overlap, other_overlap, got, own):
    count = mine.shape[0]
    keys, pieces = list(got), list(got.values())
    n, cols = count * own, pieces[0].shape[1]
    vmem = pl.BlockSpec(memory_space=pltpu.VMEM)
    return pl.pallas_call(
        functools.partial(project_kernel, count, keys),
        out_shape=[
            jax.ShapeDtypeStruct((own, cols), jnp.bfloat16),
            jax.ShapeDtypeStruct((2 * overlap.shape[0], cols), jnp.bfloat16),
        ],
        in_specs=[pl.BlockSpec(memory_space=pltpu.SMEM)] * 2
        + [vmem] * 4
        + [pl.BlockSpec(memory_space=pl.ANY)] * len(pieces),
        out_specs=[vmem, vmem],
        scratch_shapes=[
            pltpu.VMEM((n, cols), jnp.bfloat16),
            pltpu.VMEM((n, n), jnp.float32),
            pltpu.VMEM((n, n), jnp.float32),
            pltpu.VMEM((BLK, BLK), jnp.float32),
            pltpu.VMEM((BLK, BLK), jnp.float32),
            pltpu.VMEM((BLK, n), jnp.float32),
            pltpu.SemaphoreType.DMA((len(pieces),)),
        ],
        name="project",
    )(band[None], core[None], mine, other, overlap, other_overlap, *pieces)


def ring(shard, left):
    count = lax.axis_size("band")
    ways = {s: [(i, (i + s) % count) for i in range(count)] for s in (1, -1)}
    mid = shard.shape[0] // 2
    far = count // 2
    longer = ((1, 0), (-1, 1))

    def dot(piece):
        return lax.dot_general(
            left, piece, (((1,), (1,)), ((), ())), preferred_element_type=jnp.float32
        )

    got = {(0, h * mid, mid): shard[h * mid : (h + 1) * mid] for h in range(2)}
    parts = {key: dot(x) for key, x in got.items()}
    chains = {(way, h): [(0, h * mid, mid)] for way, h in longer + ((1, 1), (-1, 0))}
    for s in range(1, far + 1):
        for (way, h), keys in chains.items():
            if s == far and (way, h) not in longer:
                continue
            x = got[keys[-1]]
            if s > 1 or (way, h) not in longer:
                before = keys[max(s - 2, 0)]
                x, parts[before] = lax.optimization_barrier((x, parts[before]))
            key = ((keys[-1][0] - way) % count, h * mid, mid)
            got[key] = lax.ppermute(x, "band", ways[way])
            keys.append(key)
        if s > 1:
            for (way, h), keys in chains.items():
                parts[keys[s - 1]] = dot(got[keys[s - 1]])
    for way, h in longer:
        keys = chains[way, h]
        parts[keys[far]] = dot(got[keys[far]])
    return got, parts


def to_all(shard, axis):
    count = lax.axis_size(axis)
    return lax.all_to_all(
        jnp.broadcast_to(shard[None], (count, *shard.shape)), axis, 0, 0, tiled=True
    )


def shards(orbitals, kernel, block_vectors):
    band, core, count = lax.axis_index("band"), lax.axis_index("core"), lax.axis_size("band")
    total = orbitals.shape[1] * lax.axis_size("y") * lax.axis_size("core")
    own, mine = orbitals.shape[0], block_vectors.shape[0]
    ho, hb = own // 2, mine // 2
    far = count // 2
    swap = [(0, 1), (1, 0)]

    weighted = (-(orbitals.astype(jnp.float32) * kernel[None, :])).astype(jnp.bfloat16)
    left = jnp.concatenate(
        [orbitals[:ho], block_vectors[:hb], orbitals[ho:], block_vectors[hb:]], axis=0
    )
    got, parts = ring(weighted, left)

    order = sorted(parts, key=lambda key: ((key[0] - far) % count, key[1]))
    partial = jnp.concatenate([parts[key] for key in order], axis=1)
    n = own * count
    rows = ho + hb
    kept = lax.dynamic_slice_in_dim(partial, core * rows, rows, 0)
    sent = lax.dynamic_slice_in_dim(partial, (1 - core) * rows, rows, 0)
    kept = kept + lax.ppermute(sent, "core", swap)

    used = -(-(far + 1) * own // BLK) * BLK
    fold = ho // hb
    cols = n // fold
    packed = jnp.concatenate(
        [
            kept[:ho, :used],
            jnp.concatenate([kept[ho:, i * cols : (i + 1) * cols] for i in range(fold)], axis=0),
        ],
        axis=1,
    )
    summed = to_all(packed.astype(jnp.bfloat16), "y").astype(jnp.float32).sum(axis=0) / total
    margin = to_all((-summed[:, :used]).astype(jnp.bfloat16), "band")
    other_margin = lax.ppermute(margin, "core", swap)
    overlap = jnp.concatenate(
        [summed[i * hb : (i + 1) * hb, used:] for i in range(fold)], axis=1
    )
    other = lax.ppermute(overlap, "core", swap)
    return tuple(project(band, core, margin, other_margin, overlap, other, got, own))


def solution(mesh):
    images, ga, bands = (mesh.shape[a] for a in ("img", "ga", "band"))
    split_mesh = Mesh(
        mesh.devices.reshape(images, ga // 2, 2, bands), ("img", "y", "core", "band")
    )
    rows, cols = ("img", "band"), ("y", "core")

    return jax.shard_map(
        shards,
        mesh=split_mesh,
        in_specs=(P(rows, cols), P(cols), P(rows, cols)),
        out_specs=(P(rows, cols), P(rows, cols)),
        check_vma=False,
    )
```

```python
import functools

import jax
import jax.numpy as jnp
from jax import lax
from jax.experimental import pallas as pl
from jax.experimental.pallas import tpu as pltpu
from jax.sharding import Mesh
from jax.sharding import PartitionSpec as P


SUB = 8
BLK = 128
TILE = 512
NEAR = 2


def split(a):
    hi = a.astype(jnp.bfloat16)
    return hi, (a - hi.astype(jnp.float32)).astype(jnp.bfloat16)


def dot3(a, b, dims):
    (ah, al), (bh, bl) = a, b
    dot = functools.partial(
        lax.dot_general, dimension_numbers=(dims, ((), ())), preferred_element_type=jnp.float32
    )
    return dot(ah, bh) + (dot(ah, bl) + dot(al, bh))


def dot1(a, b, dims):
    a, b = a.astype(jnp.bfloat16), b.astype(jnp.bfloat16)
    return lax.dot_general(a, b, (dims, ((), ())), preferred_element_type=jnp.float32)


def dot2(a, b, dims):
    both = dot1(jnp.concatenate(split(a), axis=0), b, dims)
    return both[: a.shape[0]] + both[a.shape[0] :]


def wide(x):
    return jnp.broadcast_to(x, (SUB, BLK))


def lanes(x, k):
    return [wide(x[:, k + j : k + j + 1]) for j in range(SUB)]


def total_of(terms):
    while len(terms) > 1:
        odd = [terms[-1]] if len(terms) % 2 else []
        terms = [a + b for a, b in zip(terms[::2], terms[1::2])] + odd
    return terms[0]


def around(x, before, after):
    parts = [jnp.zeros((before, x.shape[1]), x.dtype), x, jnp.zeros((after, x.shape[1]), x.dtype)]
    return jnp.concatenate([part for part in parts if part.shape[0]], axis=0)


def inverse_of_factor(rows, inv):
    sub = lax.broadcasted_iota(jnp.int32, (SUB, BLK), 0)
    at = [sub == j for j in range(SUB)]
    cols = lanes(rows[0], 0)
    for p in range(len(rows)):
        k = p * SUB
        v, g = rows[p], inv[p]
        last = p + 1 == len(rows)
        if not last:
            ahead, below = lanes(rows[p + 1], k + SUB), lanes(rows[p + 1], k)
        out, unit, recips = g, {}, []
        for j in range(SUB):
            pivot, cj = wide(cols[j][j : j + 1]), cols[j]
            recip = 1.0 / pivot
            recips.append(recip)
            for m in range(j + 1, SUB):
                t = wide(cols[m][j : j + 1]) * recip
                unit[j, m] = t
                cols[m] = jnp.where(at[j], t, cols[m] - cj * t)
            gj = wide(g[j : j + 1])
            out = jnp.where(at[j], gj * lax.rsqrt(pivot), out)
            vj, gj = wide(v[j : j + 1]) * recip, gj * recip
            v = jnp.where(at[j], vj, v - cj * vj)
            g = jnp.where(at[j], gj, g - cj * gj)
        inv[p] = out
        if last:
            break
        lower = list(below)
        for j in range(SUB):
            for m in range(j + 1, SUB):
                lower[m] = lower[m] - lower[j] * unit[j, m]
        scaled = [lower[j] * recips[j] for j in range(SUB)]
        cols = [
            ahead[m] - total_of([lower[j] * wide(scaled[j][m : m + 1]) for j in range(SUB)])
            for m in range(SUB)
        ]
        far = min(p + 1 + NEAR, len(rows))
        if far < len(rows):
            pivots = jnp.concatenate([v, g], axis=1)
            zeros = jnp.zeros_like(pivots)
            pivots = [zeros, pivots] if p % 2 else [pivots, zeros]
            first = p // 2 * 2 * SUB
            pivots = jnp.concatenate(pivots, axis=0).astype(jnp.bfloat16)
            pivots = around(pivots, first, BLK - first - 2 * SUB)
            taken = dot1(jnp.concatenate(rows[far:], axis=0), pivots, ((1,), (0,)))
        vs = [wide(v[j : j + 1]) for j in range(SUB)]
        gs = [wide(g[j : j + 1]) for j in range(SUB)]
        for q in range(p + 1, len(rows)):
            if q < far:
                c = below if q == p + 1 else lanes(rows[q], k)
                rows[q] = rows[q] - total_of([c[j] * vs[j] for j in range(SUB)])
                inv[q] = inv[q] - total_of([c[j] * gs[j] for j in range(SUB)])
            else:
                i = (q - far) * SUB
                rows[q] = rows[q] - taken[i : i + SUB, :BLK]
                inv[q] = inv[q] - taken[i : i + SUB, BLK:]
    return inv


def eliminate(a, d_ref, g_ref, r_ref):
    blocks = a.shape[0] // BLK
    row = lax.broadcasted_iota(jnp.int32, (SUB, BLK), 0)
    col = lax.broadcasted_iota(jnp.int32, (SUB, BLK), 1)
    groups = range(BLK // SUB)
    rows_of = ((0,), (0,))

    def block(i):
        return pl.ds(pl.multiple_of(i * BLK, BLK), BLK)

    d_ref[...] = a[:BLK, :BLK]
    r_ref[...] = jnp.zeros(r_ref.shape, jnp.float32)

    def step(b, _):
        rows = [d_ref[SUB * i : SUB * (i + 1), :] for i in groups]
        inv = [jnp.where(col == row + SUB * i, 1.0, 0.0) for i in groups]
        for i, g in enumerate(inverse_of_factor(rows, inv)):
            g_ref[SUB * i : SUB * (i + 1), :] = g
        r = r_ref[...].astype(jnp.bfloat16)
        before = block(lax.rem(b + blocks - 1, blocks))
        for i in range(blocks - 1):
            them = block(lax.rem(b + i, blocks))
            live = jnp.logical_and(b > 0, b + i < blocks)
            factor = jnp.where(live, r_ref[:, them], 0.0)
            a[them, before] = jnp.where(live, 0.0, a[them, before])
            a[them, :] = a[them, :] - dot1(factor, r, rows_of)
        here, after = block(b), block(jnp.minimum(b + 1, blocks - 1))
        g = g_ref[...]
        r_ref[...] = dot3(split(g), split(a[here, :]), ((1,), (0,)))
        factor = r_ref[:, after]
        d_ref[...] = a[after, after] - dot1(factor, factor, rows_of)
        r_ref[:, here] = g
        a[here, :] = r_ref[...]
        return 0

    lax.fori_loop(0, blocks, step, 0)


def project_kernel(count, keys, *refs):
    pieces = refs[6 : 6 + len(keys)]
    band_ref, core_ref, mine_ref, other_ref, s_ref, s_other_ref = refs[:6]
    p_ref, x_ref, w_ref, a_ref, b_ref, d_ref, g_ref, r_ref, sem = refs[6 + len(keys) :]
    n, own = a_ref.shape[0], p_ref.shape[0]
    half = own // 2
    band, core = band_ref[0], core_ref[0]

    copies = []
    for i, ((distance, first, rows), piece) in enumerate(zip(keys, pieces)):
        to = pl.multiple_of(lax.rem(band + distance, count) * own + first, SUB)
        copies.append(pltpu.make_async_copy(piece, w_ref.at[pl.ds(to, rows), :], sem.at[i]))
        copies[-1].start()

    far = count // 2
    used = (far + 1) * own
    lane = lax.broadcasted_iota(jnp.int32, (half, mine_ref.shape[2]), 1)
    twice = (lane < own) | (lane >= far * own)
    weight = jnp.where(lane < used, jnp.where(twice, 0.5, 1.0), 0.0)
    pad = jnp.zeros((half, n - mine_ref.shape[2]), jnp.float32)
    for x in range(count):
        for h in range(2):
            mine, other = mine_ref[x].astype(jnp.float32), other_ref[x].astype(jnp.float32)
            rows = jnp.where(core == h, mine, other)
            rows = jnp.where(lane < used, rows, 0.0) * weight
            rows = jnp.concatenate([rows, pad], axis=1)
            shift = ((x - far) * own) % n
            if shift:
                rows = pltpu.roll(rows, shift, 1)
            at = x * own + h * half
            b_ref[at : at + half, :] = rows
    for i in range(0, n, BLK):
        for j in range(0, n, BLK):
            a_ref[i : i + BLK, j : j + BLK] = (
                b_ref[i : i + BLK, j : j + BLK] + b_ref[j : j + BLK, i : i + BLK].T
            )

    eliminate(a_ref, d_ref, g_ref, r_ref)

    row = lax.broadcasted_iota(jnp.int32, (n, n), 0)
    col = lax.broadcasted_iota(jnp.int32, (n, n), 1)
    inverse = jnp.where(row >= col, a_ref[...], 0.0).astype(jnp.bfloat16)
    overlap = jnp.concatenate(
        [
            jnp.where(core == 0, s_ref[...], s_other_ref[...]),
            jnp.where(core == 0, s_other_ref[...], s_ref[...]),
        ],
        axis=0,
    )
    overlap = pltpu.roll(overlap, lax.rem(band + far, count) * own, 1)
    coupling = dot2(overlap, inverse, ((1,), (1,)))
    applied = -dot2(coupling, inverse, ((1,), (0,)))
    first = pl.multiple_of(band * own, SUB)
    own_row = first + lax.broadcasted_iota(jnp.int32, (own, n), 0)
    own_rows = jnp.where(own_row >= col[:own], a_ref[pl.ds(first, own), :], 0.0)
    coefs = jnp.concatenate([own_rows, applied], axis=0).astype(jnp.bfloat16)

    for copy in copies:
        copy.wait()
    for at in range(0, w_ref.shape[1], TILE):
        out = jnp.dot(coefs, w_ref[:, at : at + TILE], preferred_element_type=jnp.float32)
        out = out.astype(jnp.bfloat16)
        p_ref[:, at : at + TILE] = out[:own]
        x_ref[:, at : at + TILE] = out[own:]


def project(band, core, mine, other, overlap, other_overlap, got, own):
    count = mine.shape[0]
    keys, pieces = list(got), list(got.values())
    n, cols = count * own, pieces[0].shape[1]
    vmem = pl.BlockSpec(memory_space=pltpu.VMEM)
    return pl.pallas_call(
        functools.partial(project_kernel, count, keys),
        out_shape=[
            jax.ShapeDtypeStruct((own, cols), jnp.bfloat16),
            jax.ShapeDtypeStruct((2 * overlap.shape[0], cols), jnp.bfloat16),
        ],
        in_specs=[pl.BlockSpec(memory_space=pltpu.SMEM)] * 2
        + [vmem] * 4
        + [pl.BlockSpec(memory_space=pl.ANY)] * len(pieces),
        out_specs=[vmem, vmem],
        scratch_shapes=[
            pltpu.VMEM((n, cols), jnp.bfloat16),
            pltpu.VMEM((n, n), jnp.float32),
            pltpu.VMEM((n, n), jnp.float32),
            pltpu.VMEM((BLK, BLK), jnp.float32),
            pltpu.VMEM((BLK, BLK), jnp.float32),
            pltpu.VMEM((BLK, n), jnp.float32),
            pltpu.SemaphoreType.DMA((len(pieces),)),
        ],
        name="project",
    )(band[None], core[None], mine, other, overlap, other_overlap, *pieces)


def ring(shard, left):
    count = lax.axis_size("band")
    ways = {s: [(i, (i + s) % count) for i in range(count)] for s in (1, -1)}
    mid = shard.shape[0] // 2
    far = count // 2
    longer = ((1, 0), (-1, 1))

    def dot(piece):
        return lax.dot_general(
            left, piece, (((1,), (1,)), ((), ())), preferred_element_type=jnp.float32
        )

    got = {(0, h * mid, mid): shard[h * mid : (h + 1) * mid] for h in range(2)}
    parts = {key: dot(x) for key, x in got.items()}
    chains = {(way, h): [(0, h * mid, mid)] for way, h in longer + ((1, 1), (-1, 0))}
    for s in range(1, far + 1):
        for (way, h), keys in chains.items():
            if s == far and (way, h) not in longer:
                continue
            x = got[keys[-1]]
            key = ((keys[-1][0] - way) % count, h * mid, mid)
            got[key] = lax.ppermute(x, "band", ways[way])
            keys.append(key)
        if s > 1:
            for (way, h), keys in chains.items():
                parts[keys[s - 1]] = dot(got[keys[s - 1]])
    for way, h in longer:
        keys = chains[way, h]
        parts[keys[far]] = dot(got[keys[far]])
    return got, parts


def to_all(shard, axis):
    count = lax.axis_size(axis)
    return lax.all_to_all(
        jnp.broadcast_to(shard[None], (count, *shard.shape)), axis, 0, 0, tiled=True
    )


def shards(orbitals, kernel, block_vectors):
    band, core, count = lax.axis_index("band"), lax.axis_index("core"), lax.axis_size("band")
    total = orbitals.shape[1] * lax.axis_size("y") * lax.axis_size("core")
    own, mine = orbitals.shape[0], block_vectors.shape[0]
    ho, hb = own // 2, mine // 2
    far = count // 2
    swap = [(0, 1), (1, 0)]

    weighted = (-(orbitals.astype(jnp.float32) * kernel[None, :])).astype(jnp.bfloat16)
    left = jnp.concatenate(
        [orbitals[:ho], block_vectors[:hb], orbitals[ho:], block_vectors[hb:]], axis=0
    )
    got, parts = ring(weighted, left)

    n = own * count
    partial = jnp.zeros((left.shape[0], n), jnp.float32)
    for (distance, row, _), part in parts.items():
        at = (distance - far) % count * own + row
        partial = lax.dynamic_update_slice_in_dim(partial, part, at, 1)
    rows = ho + hb
    kept = lax.dynamic_slice_in_dim(partial, core * rows, rows, 0)
    sent = lax.dynamic_slice_in_dim(partial, (1 - core) * rows, rows, 0)
    kept = kept + lax.ppermute(sent, "core", swap)

    used = -(-(far + 1) * own // BLK) * BLK
    fold = ho // hb
    cols = n // fold
    packed = jnp.concatenate(
        [
            kept[:ho, :used],
            jnp.concatenate([kept[ho:, i * cols : (i + 1) * cols] for i in range(fold)], axis=0),
        ],
        axis=1,
    )
    summed = to_all(packed.astype(jnp.bfloat16), "y").astype(jnp.float32).sum(axis=0) / total
    margin = to_all((-summed[:, :used]).astype(jnp.bfloat16), "band")
    other_margin = lax.ppermute(margin, "core", swap)
    overlap = jnp.concatenate(
        [summed[i * hb : (i + 1) * hb, used:] for i in range(fold)], axis=1
    )
    other = lax.ppermute(overlap, "core", swap)
    return tuple(project(band, core, margin, other_margin, overlap, other, got, own))


def solution(mesh):
    images, ga, bands = (mesh.shape[a] for a in ("img", "ga", "band"))
    split_mesh = Mesh(
        mesh.devices.reshape(images, ga // 2, 2, bands), ("img", "y", "core", "band")
    )
    rows, cols = ("img", "band"), ("y", "core")

    return jax.shard_map(
        shards,
        mesh=split_mesh,
        in_specs=(P(rows, cols), P(cols), P(rows, cols)),
        out_specs=(P(rows, cols), P(rows, cols)),
        check_vma=False,
    )
```

```python
import functools

import jax
import jax.numpy as jnp
from jax import lax
from jax.experimental import pallas as pl
from jax.experimental.pallas import tpu as pltpu
from jax.sharding import Mesh
from jax.sharding import PartitionSpec as P


SUB = 8
BLK = 128
TILE = 512
NEAR = 2


def split(a):
    hi = a.astype(jnp.bfloat16)
    return hi, (a - hi.astype(jnp.float32)).astype(jnp.bfloat16)


def dot1(a, b, dims):
    a, b = a.astype(jnp.bfloat16), b.astype(jnp.bfloat16)
    return lax.dot_general(a, b, (dims, ((), ())), preferred_element_type=jnp.float32)


def dot2(a, b, dims):
    both = dot1(jnp.concatenate(split(a), axis=0), b, dims)
    return both[: a.shape[0]] + both[a.shape[0] :]


def wide(x):
    return jnp.broadcast_to(x, (SUB, BLK))


def lanes(x, k):
    return [wide(x[:, k + j : k + j + 1]) for j in range(SUB)]


def total_of(terms):
    while len(terms) > 1:
        odd = [terms[-1]] if len(terms) % 2 else []
        terms = [a + b for a, b in zip(terms[::2], terms[1::2])] + odd
    return terms[0]


def around(x, before, after):
    parts = [jnp.zeros((before, x.shape[1]), x.dtype), x, jnp.zeros((after, x.shape[1]), x.dtype)]
    return jnp.concatenate([part for part in parts if part.shape[0]], axis=0)


def inverse_of_factor(rows, inv):
    sub = lax.broadcasted_iota(jnp.int32, (SUB, BLK), 0)
    at = [sub == j for j in range(SUB)]
    cols = lanes(rows[0], 0)
    for p in range(len(rows)):
        k = p * SUB
        v, g = rows[p], inv[p]
        last = p + 1 == len(rows)
        if not last:
            ahead, below = lanes(rows[p + 1], k + SUB), lanes(rows[p + 1], k)
        out, unit, recips = g, {}, []
        for j in range(SUB):
            pivot, cj = wide(cols[j][j : j + 1]), cols[j]
            recip = 1.0 / pivot
            recips.append(recip)
            for m in range(j + 1, SUB):
                t = wide(cols[m][j : j + 1]) * recip
                unit[j, m] = t
                cols[m] = jnp.where(at[j], t, cols[m] - cj * t)
            gj = wide(g[j : j + 1])
            out = jnp.where(at[j], gj * lax.rsqrt(pivot), out)
            vj, gj = wide(v[j : j + 1]) * recip, gj * recip
            v = jnp.where(at[j], vj, v - cj * vj)
            g = jnp.where(at[j], gj, g - cj * gj)
        inv[p] = out
        if last:
            break
        lower = list(below)
        for j in range(SUB):
            for m in range(j + 1, SUB):
                lower[m] = lower[m] - lower[j] * unit[j, m]
        scaled = [lower[j] * recips[j] for j in range(SUB)]
        cols = [
            ahead[m] - total_of([lower[j] * wide(scaled[j][m : m + 1]) for j in range(SUB)])
            for m in range(SUB)
        ]
        far = min(p + 1 + NEAR, len(rows))
        if far < len(rows):
            pivots = jnp.concatenate([v, g], axis=1)
            zeros = jnp.zeros_like(pivots)
            pivots = [zeros, pivots] if p % 2 else [pivots, zeros]
            first = p // 2 * 2 * SUB
            pivots = jnp.concatenate(pivots, axis=0).astype(jnp.bfloat16)
            pivots = around(pivots, first, BLK - first - 2 * SUB)
            taken = dot1(jnp.concatenate(rows[far:], axis=0), pivots, ((1,), (0,)))
        vs = [wide(v[j : j + 1]) for j in range(SUB)]
        gs = [wide(g[j : j + 1]) for j in range(SUB)]
        for q in range(p + 1, len(rows)):
            if q < far:
                c = below if q == p + 1 else lanes(rows[q], k)
                rows[q] = rows[q] - total_of([c[j] * vs[j] for j in range(SUB)])
                inv[q] = inv[q] - total_of([c[j] * gs[j] for j in range(SUB)])
            else:
                i = (q - far) * SUB
                rows[q] = rows[q] - taken[i : i + SUB, :BLK]
                inv[q] = inv[q] - taken[i : i + SUB, BLK:]
    return inv


def eliminate(a, d_ref, g_ref, r_ref):
    blocks = a.shape[0] // BLK
    row = lax.broadcasted_iota(jnp.int32, (SUB, BLK), 0)
    col = lax.broadcasted_iota(jnp.int32, (SUB, BLK), 1)
    groups = range(BLK // SUB)
    rows_of = ((0,), (0,))

    def block(i):
        return pl.ds(pl.multiple_of(i * BLK, BLK), BLK)

    d_ref[...] = a[:BLK, :BLK]
    r_ref[...] = jnp.zeros(r_ref.shape, jnp.float32)

    def step(b, _):
        rows = [d_ref[SUB * i : SUB * (i + 1), :] for i in groups]
        inv = [jnp.where(col == row + SUB * i, 1.0, 0.0) for i in groups]
        for i, g in enumerate(inverse_of_factor(rows, inv)):
            g_ref[SUB * i : SUB * (i + 1), :] = g
        r = r_ref[...].astype(jnp.bfloat16)
        before = block(lax.rem(b + blocks - 1, blocks))
        for i in range(blocks - 1):
            them = block(lax.rem(b + i, blocks))
            live = jnp.logical_and(b > 0, b + i < blocks)
            factor = jnp.where(live, r_ref[:, them], 0.0)
            a[them, before] = jnp.where(live, 0.0, a[them, before])
            a[them, :] = a[them, :] - dot1(factor, r, rows_of)
        here, after = block(b), block(jnp.minimum(b + 1, blocks - 1))
        g = g_ref[...]
        r_ref[...] = dot2(g, a[here, :], ((1,), (0,)))
        factor = r_ref[:, after]
        d_ref[...] = a[after, after] - dot1(factor, factor, rows_of)
        r_ref[:, here] = g
        a[here, :] = r_ref[...]
        return 0

    lax.fori_loop(0, blocks, step, 0)


def project_kernel(count, keys, *refs):
    pieces = refs[6 : 6 + len(keys)]
    band_ref, core_ref, mine_ref, other_ref, s_ref, s_other_ref = refs[:6]
    p_ref, x_ref, w_ref, a_ref, b_ref, d_ref, g_ref, r_ref, sem = refs[6 + len(keys) :]
    n, own = a_ref.shape[0], p_ref.shape[0]
    half = own // 2
    band, core = band_ref[0], core_ref[0]

    copies = []
    for i, ((distance, first, rows), piece) in enumerate(zip(keys, pieces)):
        to = pl.multiple_of(lax.rem(band + distance, count) * own + first, SUB)
        copies.append(pltpu.make_async_copy(piece, w_ref.at[pl.ds(to, rows), :], sem.at[i]))
        copies[-1].start()

    far = count // 2
    used = (far + 1) * own
    lane = lax.broadcasted_iota(jnp.int32, (half, mine_ref.shape[2]), 1)
    twice = (lane < own) | (lane >= far * own)
    weight = jnp.where(lane < used, jnp.where(twice, 0.5, 1.0), 0.0)
    pad = jnp.zeros((half, n - mine_ref.shape[2]), jnp.float32)
    for x in range(count):
        for h in range(2):
            mine, other = mine_ref[x].astype(jnp.float32), other_ref[x].astype(jnp.float32)
            rows = jnp.where(core == h, mine, other)
            rows = jnp.where(lane < used, rows, 0.0) * weight
            rows = jnp.concatenate([rows, pad], axis=1)
            shift = ((x - far) * own) % n
            if shift:
                rows = pltpu.roll(rows, shift, 1)
            at = x * own + h * half
            b_ref[at : at + half, :] = rows
    for i in range(0, n, BLK):
        for j in range(0, n, BLK):
            a_ref[i : i + BLK, j : j + BLK] = (
                b_ref[i : i + BLK, j : j + BLK] + b_ref[j : j + BLK, i : i + BLK].T
            )

    eliminate(a_ref, d_ref, g_ref, r_ref)

    row = lax.broadcasted_iota(jnp.int32, (n, n), 0)
    col = lax.broadcasted_iota(jnp.int32, (n, n), 1)
    inverse = jnp.where(row >= col, a_ref[...], 0.0).astype(jnp.bfloat16)
    overlap = jnp.concatenate(
        [
            jnp.where(core == 0, s_ref[...], s_other_ref[...]),
            jnp.where(core == 0, s_other_ref[...], s_ref[...]),
        ],
        axis=0,
    )
    overlap = pltpu.roll(overlap, lax.rem(band + far, count) * own, 1)
    coupling = dot2(overlap, inverse, ((1,), (1,)))
    applied = -dot2(coupling, inverse, ((1,), (0,)))
    first = pl.multiple_of(band * own, SUB)
    own_row = first + lax.broadcasted_iota(jnp.int32, (own, n), 0)
    own_rows = jnp.where(own_row >= col[:own], a_ref[pl.ds(first, own), :], 0.0)
    coefs = jnp.concatenate([own_rows, applied], axis=0).astype(jnp.bfloat16)

    for copy in copies:
        copy.wait()
    for at in range(0, w_ref.shape[1], TILE):
        out = jnp.dot(coefs, w_ref[:, at : at + TILE], preferred_element_type=jnp.float32)
        out = out.astype(jnp.bfloat16)
        p_ref[:, at : at + TILE] = out[:own]
        x_ref[:, at : at + TILE] = out[own:]


def project(band, core, mine, other, overlap, other_overlap, got, own):
    count = mine.shape[0]
    keys, pieces = list(got), list(got.values())
    n, cols = count * own, pieces[0].shape[1]
    vmem = pl.BlockSpec(memory_space=pltpu.VMEM)
    return pl.pallas_call(
        functools.partial(project_kernel, count, keys),
        out_shape=[
            jax.ShapeDtypeStruct((own, cols), jnp.bfloat16),
            jax.ShapeDtypeStruct((2 * overlap.shape[0], cols), jnp.bfloat16),
        ],
        in_specs=[pl.BlockSpec(memory_space=pltpu.SMEM)] * 2
        + [vmem] * 4
        + [pl.BlockSpec(memory_space=pl.ANY)] * len(pieces),
        out_specs=[vmem, vmem],
        scratch_shapes=[
            pltpu.VMEM((n, cols), jnp.bfloat16),
            pltpu.VMEM((n, n), jnp.float32),
            pltpu.VMEM((n, n), jnp.float32),
            pltpu.VMEM((BLK, BLK), jnp.float32),
            pltpu.VMEM((BLK, BLK), jnp.float32),
            pltpu.VMEM((BLK, n), jnp.float32),
            pltpu.SemaphoreType.DMA((len(pieces),)),
        ],
        name="project",
    )(band[None], core[None], mine, other, overlap, other_overlap, *pieces)


def ring(shard, left):
    count = lax.axis_size("band")
    ways = {s: [(i, (i + s) % count) for i in range(count)] for s in (1, -1)}
    mid = shard.shape[0] // 2
    far = count // 2
    longer = ((1, 0), (-1, 1))

    def dot(piece):
        return lax.dot_general(
            left, piece, (((1,), (1,)), ((), ())), preferred_element_type=jnp.float32
        )

    got = {(0, h * mid, mid): shard[h * mid : (h + 1) * mid] for h in range(2)}
    parts = {key: dot(x) for key, x in got.items()}
    chains = {(way, h): [(0, h * mid, mid)] for way, h in longer + ((1, 1), (-1, 0))}
    for s in range(1, far + 1):
        for (way, h), keys in chains.items():
            if s == far and (way, h) not in longer:
                continue
            x = got[keys[-1]]
            key = ((keys[-1][0] - way) % count, h * mid, mid)
            got[key] = lax.ppermute(x, "band", ways[way])
            keys.append(key)
        if s > 1:
            for (way, h), keys in chains.items():
                parts[keys[s - 1]] = dot(got[keys[s - 1]])
    for way, h in longer:
        keys = chains[way, h]
        parts[keys[far]] = dot(got[keys[far]])
    return got, parts


def to_all(shard, axis):
    count = lax.axis_size(axis)
    return lax.all_to_all(
        jnp.broadcast_to(shard[None], (count, *shard.shape)), axis, 0, 0, tiled=True
    )


def shards(orbitals, kernel, block_vectors):
    band, core, count = lax.axis_index("band"), lax.axis_index("core"), lax.axis_size("band")
    total = orbitals.shape[1] * lax.axis_size("y") * lax.axis_size("core")
    own, mine = orbitals.shape[0], block_vectors.shape[0]
    ho, hb = own // 2, mine // 2
    far = count // 2
    swap = [(0, 1), (1, 0)]

    weighted = (-(orbitals.astype(jnp.float32) * kernel[None, :])).astype(jnp.bfloat16)
    left = jnp.concatenate(
        [orbitals[:ho], block_vectors[:hb], orbitals[ho:], block_vectors[hb:]], axis=0
    )
    got, parts = ring(weighted, left)

    n = own * count
    partial = jnp.zeros((left.shape[0], n), jnp.float32)
    for (distance, row, _), part in parts.items():
        at = (distance - far) % count * own + row
        partial = lax.dynamic_update_slice_in_dim(partial, part, at, 1)
    rows = ho + hb
    kept = lax.dynamic_slice_in_dim(partial, core * rows, rows, 0)
    sent = lax.dynamic_slice_in_dim(partial, (1 - core) * rows, rows, 0)
    kept = kept + lax.ppermute(sent, "core", swap)

    used = -(-(far + 1) * own // BLK) * BLK
    fold = ho // hb
    cols = n // fold
    packed = jnp.concatenate(
        [
            kept[:ho, :used],
            jnp.concatenate([kept[ho:, i * cols : (i + 1) * cols] for i in range(fold)], axis=0),
        ],
        axis=1,
    )
    summed = to_all(packed.astype(jnp.bfloat16), "y").astype(jnp.float32).sum(axis=0) / total
    margin = to_all((-summed[:, :used]).astype(jnp.bfloat16), "band")
    other_margin = lax.ppermute(margin, "core", swap)
    overlap = jnp.concatenate(
        [summed[i * hb : (i + 1) * hb, used:] for i in range(fold)], axis=1
    )
    other = lax.ppermute(overlap, "core", swap)
    return tuple(project(band, core, margin, other_margin, overlap, other, got, own))


def solution(mesh):
    images, ga, bands = (mesh.shape[a] for a in ("img", "ga", "band"))
    split_mesh = Mesh(
        mesh.devices.reshape(images, ga // 2, 2, bands), ("img", "y", "core", "band")
    )
    rows, cols = ("img", "band"), ("y", "core")

    return jax.shard_map(
        shards,
        mesh=split_mesh,
        in_specs=(P(rows, cols), P(cols), P(rows, cols)),
        out_specs=(P(rows, cols), P(rows, cols)),
        check_vma=False,
    )
```
